8 devices in a mesh: dp: 1 (over z), row: 2 (over y), col: 4 (over x, core).
Axes of the slice: x: 2, y: 2, z: 1, core: 2. Of those that a mesh axis runs over, the one named last changes fastest.
Arguments:
- pair_rep: bfloat16 [512, 512, 128], P(('dp', 'row'), 'col')
- res_mask: int32 [512], P('dp')
- ln_gamma: float32 [128], replicated
- ln_beta: float32 [128], replicated
- w_q: bfloat16 [128, 128], replicated
- w_k: bfloat16 [128, 128], replicated
- w_v: bfloat16 [128, 128], replicated
- w_b: bfloat16 [128, 4], replicated
- w_g: bfloat16 [128, 128], replicated
- w_o: bfloat16 [128, 128], replicated
Outputs:
- output: bfloat16 [512, 512, 128], P(('dp', 'row'), 'col')
All inputs are finite; a program needn't handle non-finite values.
Results may differ from the reference program's by a relative error of at most 0.0072822.
Values are sent between devices in bfloat16 or wider.
A program may use at most 1 GiB of HBM per device.

```python
import jax
import jax.numpy as jnp
from jax import lax

N = 512
C_Z = 128
HEADS = 4
HEAD = 32
LN_EPS = 1e-5


def layer_norm(pair_rep, ln_gamma, ln_beta):
    pair_f32 = pair_rep.astype(jnp.float32)
    mean_c = jnp.mean(pair_f32, axis=-1, keepdims=True)
    centered = pair_f32 - mean_c
    var_c = jnp.mean(jnp.square(centered), axis=-1, keepdims=True)
    return (centered * lax.rsqrt(var_c + LN_EPS) * ln_gamma + ln_beta).astype(jnp.bfloat16)


def setup_inputs(seed: int = 0, part: int = 0) -> dict:
    part_key = jax.random.fold_in(jax.random.key(seed), part)
    pair_key, len_key = jax.random.split(part_key)
    weight_keys = jax.random.split(jax.random.key(seed + 1), 8)
    proj_dim = HEADS * HEAD
    in_scale = C_Z ** -0.5
    pair_rep = jax.random.normal(pair_key, (N, N, C_Z), jnp.float32).astype(jnp.bfloat16)
    seq_len = jax.random.randint(len_key, (), N // 4, N - N // 8 + 1)
    res_mask = (jnp.arange(N) < seq_len).astype(jnp.int32)
    ln_gamma = 1.0 + 0.5 * jax.random.normal(weight_keys[0], (C_Z,), jnp.float32)
    ln_beta = 0.5 * jax.random.normal(weight_keys[1], (C_Z,), jnp.float32)
    w_q = (jax.random.normal(weight_keys[2], (C_Z, proj_dim), jnp.float32) * in_scale).astype(jnp.bfloat16)
    w_k = (jax.random.normal(weight_keys[3], (C_Z, proj_dim), jnp.float32) * in_scale).astype(jnp.bfloat16)
    w_v = (jax.random.normal(weight_keys[4], (C_Z, proj_dim), jnp.float32) * in_scale).astype(jnp.bfloat16)
    w_b = (jax.random.normal(weight_keys[5], (C_Z, HEADS), jnp.float32) * in_scale).astype(jnp.bfloat16)
    w_g = (jax.random.normal(weight_keys[6], (C_Z, proj_dim), jnp.float32) * in_scale).astype(jnp.bfloat16)
    w_o = (jax.random.normal(weight_keys[7], (proj_dim, C_Z), jnp.float32) * (4.0 * proj_dim ** -0.5)).astype(jnp.bfloat16)
    return {'pair_rep': pair_rep, 'res_mask': res_mask, 'ln_gamma': ln_gamma, 'ln_beta': ln_beta, 'w_q': w_q, 'w_k': w_k, 'w_v': w_v, 'w_b': w_b, 'w_g': w_g, 'w_o': w_o}


def reference(pair_rep, res_mask, ln_gamma, ln_beta, w_q, w_k, w_v, w_b, w_g, w_o):
    proj_dim = HEADS * HEAD
    normed = layer_norm(pair_rep, ln_gamma, ln_beta)
    pair_bias = jnp.dot(normed.reshape(N * N, C_Z), w_b, preferred_element_type=jnp.float32).astype(jnp.bfloat16)
    key_bias = jnp.where(res_mask > 0, 0.0, -1e9).astype(jnp.float32)
    full_bias = pair_bias.reshape(N, N, HEADS).astype(jnp.float32) + key_bias[None, :, None]

    def one_row(row_args):
        pair_row, normed_row = row_args
        queries = (jnp.dot(normed_row, w_q, preferred_element_type=jnp.float32) * HEAD ** -0.5).astype(jnp.bfloat16)
        key_row = jnp.dot(normed_row, w_k, preferred_element_type=jnp.float32).astype(jnp.bfloat16)
        val_row = jnp.dot(normed_row, w_v, preferred_element_type=jnp.float32).astype(jnp.bfloat16)
        gate_vals = jax.nn.sigmoid(jnp.dot(normed_row, w_g, preferred_element_type=jnp.float32))
        logits = jnp.einsum('jhd,khd->jkh', queries.reshape(N, HEADS, HEAD).astype(jnp.float32), key_row.reshape(N, HEADS, HEAD).astype(jnp.float32)) + full_bias
        weights = jax.nn.softmax(logits, axis=1)
        attended = jnp.einsum('jkh,khd->jhd', weights, val_row.reshape(N, HEADS, HEAD).astype(jnp.float32))
        gated_out = (gate_vals * attended.reshape(N, proj_dim)).astype(jnp.bfloat16)
        update = jnp.dot(gated_out, w_o, preferred_element_type=jnp.float32)
        return (pair_row.astype(jnp.float32) + update).astype(jnp.bfloat16)

    return lax.map(one_row, (pair_rep, normed))
```

```python
import functools

import jax
import jax.numpy as jnp
from jax import lax
from jax.experimental import pallas as pl
from jax.experimental.pallas import tpu as pltpu
from jax.sharding import PartitionSpec as P

LN_EPS = 1e-5
CHUNKS = (32, 48, 48, 48, 32, 24, 16, 8)
ROWS_STEP = 8


def norm_kernel(z_ref, gamma_ref, beta_ref, wb_ref, a_ref, b_ref):
    rows, cols, chan = z_ref.shape
    z = z_ref[...].reshape(rows * cols, chan)
    ones = jnp.full((chan, chan), 1.0 / chan, jnp.bfloat16)
    mean = jnp.dot(z, ones, preferred_element_type=jnp.float32)
    centered = z.astype(jnp.float32) - mean
    var = jnp.mean(centered * centered, axis=-1, keepdims=True)
    a = (centered * lax.rsqrt(var + LN_EPS) * gamma_ref[...] + beta_ref[...]).astype(jnp.bfloat16)
    a_ref[...] = a.reshape(rows, cols, chan)
    b = lax.dot_general(wb_ref[...], a, (((1,), (1,)), ((), ())), preferred_element_type=jnp.float32)
    for r in range(rows):
        b_ref[r] = b[:, r * cols:(r + 1) * cols]


def normalize(z, gamma, beta, wb_t, start, rows):
    cols, chan = z.shape[1:]
    step = min(rows, ROWS_STEP)
    first = start // step
    whole = lambda shape: pl.BlockSpec(shape, lambda i: (0,) * len(shape))
    return pl.pallas_call(
        norm_kernel,
        grid=(rows // step,),
        in_specs=[
            pl.BlockSpec((step, cols, chan), lambda i: (first + i, 0, 0)),
            whole((1, chan)), whole((1, chan)), whole(wb_t.shape),
        ],
        out_specs=[
            pl.BlockSpec((step, cols, chan), lambda i: (i, 0, 0)),
            pl.BlockSpec((step, wb_t.shape[0], cols), lambda i: (i, 0, 0)),
        ],
        out_shape=[
            jax.ShapeDtypeStruct((rows, cols, chan), jnp.bfloat16),
            jax.ShapeDtypeStruct((rows, wb_t.shape[0], cols), jnp.float32),
        ],
        cost_estimate=pl.CostEstimate(flops=rows * cols * chan * 300, bytes_accessed=rows * cols * chan * 4, transcendentals=0),
        name="norm",
    )(z, gamma, beta, wb_t)


def attend_kernel(heads, aliased, *refs):
    ao_ref, ap_ref, ax_ref, ad_ref, z_ref, bias_ref, wq_ref, wk_ref, wv_ref, wg_ref, wo_ref = refs[:11]
    out_ref = refs[12] if aliased else refs[11]
    step, cols, chan = ao_ref.shape
    dim = chan // heads
    f32, bf16 = jnp.float32, jnp.bfloat16
    nn = (((1,), (0,)), ((), ()))
    nt = (((1,), (1,)), ((), ()))
    tn = (((0,), (0,)), ((), ()))
    dot = functools.partial(lax.dot_general, preferred_element_type=f32)
    lane_head = lax.broadcasted_iota(jnp.int32, (cols, chan), 1) // dim

    def one_row(t):
        own = ao_ref[t]
        keys_in = jnp.concatenate([own, ap_ref[t], ax_ref[t], ad_ref[t]], axis=0)
        k = dot(keys_in, wk_ref[...], nn).astype(bf16)
        v_t = dot(wv_ref[...], keys_in, nt).astype(bf16)
        q = (dot(own, wq_ref[...], nn) * dim ** -0.5).astype(bf16)
        q_all = jnp.concatenate([jnp.where(lane_head == h, q, jnp.zeros_like(q)) for h in range(heads)], axis=0)
        gate = jax.nn.sigmoid(dot(wg_ref[...], own, nt))
        outs = []
        for g in range(heads // 2):
            s = dot(k, q_all[2 * g * cols:(2 * g + 2) * cols], nt) + bias_ref[:, 2 * g * cols:(2 * g + 2) * cols]
            m = jnp.max(s, axis=0, keepdims=True)
            p = jnp.exp(s - m)
            inv = 1.0 / jnp.sum(p, axis=0, keepdims=True)
            o = dot(v_t[2 * g * dim:(2 * g + 2) * dim], p.astype(bf16), nn)
            outs.append(o[:dim, :cols] * inv[:, :cols])
            outs.append(o[dim:, cols:] * inv[:, cols:])
        gated = (jnp.concatenate(outs, axis=0) * gate).astype(bf16)
        update = dot(gated, wo_ref[...], tn)
        out_ref[t] = (z_ref[t].astype(f32) + update).astype(bf16)

    def body(i, carry):
        one_row(2 * i)
        one_row(2 * i + 1)
        return carry

    lax.fori_loop(0, step // 2, body, 0)


def attend(heads, blocks, z, bias, weights, prev, start, rows):
    total, cols, chan = z.shape
    step = ROWS_STEP
    first = start // step
    here = pl.BlockSpec((step, cols, chan), lambda i: (i, 0, 0))
    there = pl.BlockSpec((step, cols, chan), lambda i: (first + i, 0, 0))
    whole = lambda shape: pl.BlockSpec(shape, lambda i: (0,) * len(shape))
    args = list(blocks) + [z, bias] + list(weights)
    specs = [here] * 4 + [there, whole(bias.shape)] + [whole(w.shape) for w in weights]
    alias = {}
    if prev is not None:
        alias = {len(args): 0}
        args.append(prev)
        specs.append(pl.BlockSpec(memory_space=pl.ANY))
    return pl.pallas_call(
        functools.partial(attend_kernel, heads, prev is not None),
        grid=(rows // step,),
        in_specs=specs,
        out_specs=there,
        out_shape=jax.ShapeDtypeStruct(z.shape, z.dtype),
        input_output_aliases=alias,
        compiler_params=pltpu.CompilerParams(vmem_limit_bytes=40 * 1024 * 1024),
        cost_estimate=pl.CostEstimate(flops=rows * cols * chan * 16000, bytes_accessed=rows * cols * chan * 12, transcendentals=0),
        name="attend",
    )(*args)


def solution(mesh):
    tile_spec = P(('dp', 'row'), 'col', None)
    num_rows, num_cols = mesh.shape['row'], mesh.shape['col']
    x_pairs = [(c, c ^ 2) for c in range(num_cols)]
    core_pairs = [(c, c ^ 1) for c in range(num_cols)]

    def bias_pairs(m):
        pairs = []
        for r in range(num_rows):
            for c in range(num_cols):
                e = c ^ m
                pairs.append((r * num_cols + c, (e >> 1) * num_cols + 2 * r + (e & 1)))
        return pairs

    def per_device(z, res_mask, ln_gamma, ln_beta, w_q, w_k, w_v, w_b, w_g, w_o):
        row_len, cols, chan = z.shape
        heads = w_b.shape[1]
        row_idx, col_idx = lax.axis_index('row'), lax.axis_index('col')
        gamma, beta = ln_gamma.reshape(1, chan), ln_beta.reshape(1, chan)
        wb_t = jnp.pad(w_b.T, ((0, 8 - heads), (0, 0)))
        weights = (w_q, w_k, w_v.T, w_g.T, w_o)

        starts = [sum(CHUNKS[:i]) for i in range(len(CHUNKS))]
        own, bias_parts = [], []
        for start, rows in zip(starts, CHUNKS):
            a, b = normalize(z, gamma, beta, wb_t, start, rows)
            own.append(a)
            bias_parts.append(b[:, :heads].astype(jnp.bfloat16))
        bias_tile = jnp.concatenate(bias_parts, axis=0)
        halves = bias_tile.reshape(2, row_len // 2, heads, cols)

        far = [lax.ppermute(own[0], 'col', x_pairs)]
        got = []
        for m in range(4):
            half = lax.dynamic_index_in_dim(halves, (col_idx ^ m) & 1, 0, keepdims=False)
            got.append(lax.ppermute(half, ('row', 'col'), bias_pairs(m)))
        same = (col_idx >> 1) == row_idx
        rel = jnp.stack([jnp.where(same, got[p], got[p ^ 2]) for p in range(4)])
        mask_blocks = res_mask.reshape(num_cols, cols)
        key_mask = jnp.stack([lax.dynamic_index_in_dim(mask_blocks, col_idx ^ p, 0, keepdims=False) for p in range(4)])
        key_bias = jnp.where(key_mask > 0, 0.0, -1e9).astype(jnp.float32)
        bias = jnp.transpose(rel, (0, 3, 2, 1)).astype(jnp.float32) + key_bias[:, :, None, None]
        bias = bias.reshape(4 * cols, heads * cols)

        for i in range(1, len(CHUNKS)):
            far.append(lax.ppermute(own[i], 'col', x_pairs))
        near = [lax.ppermute(a, 'col', core_pairs) for a in own]
        out = None
        for i, (start, rows) in enumerate(zip(starts, CHUNKS)):
            diag = lax.ppermute(far[i], 'col', core_pairs)
            out = attend(heads, (own[i], near[i], far[i], diag), z, bias, weights, out, start, rows)
        return out

    return jax.shard_map(per_device, mesh=mesh, in_specs=(tile_spec, P('dp'), P(), P(), P(), P(), P(), P(), P(), P()), out_specs=tile_spec, check_vma=False)
```

```python
import functools

import jax
import jax.numpy as jnp
from jax import lax
from jax.experimental import pallas as pl
from jax.experimental.pallas import tpu as pltpu
from jax.sharding import PartitionSpec as P


LN_EPS = 1e-5
CHUNKS = (32, 32, 48, 48, 48, 16, 16, 16)
NORM_ROWS = 16
ATTEND_ROWS = 8
SCORE_BOUND = 1e8
NN = (((1,), (0,)), ((), ()))
NT = (((1,), (1,)), ((), ()))
f32, bf16 = jnp.float32, jnp.bfloat16
dot = functools.partial(lax.dot_general, preferred_element_type=f32)
VMEM_LIMIT = pltpu.CompilerParams(vmem_limit_bytes=60 * 1024 * 1024)


def whole(shape):
    return pl.BlockSpec(shape, lambda *_: (0,) * len(shape))


def bound_kernel(heads, gamma_ref, beta_ref, wq_ref, wk_ref, wb_ref, out_ref):
    chan = gamma_ref.shape[1]
    dim = chan // heads
    reach = jnp.broadcast_to(jnp.abs(gamma_ref[...]) * chan ** 0.5 + jnp.abs(beta_ref[...]), (8, chan)) * 1.05
    q = jnp.dot(reach, jnp.abs(wq_ref[...].astype(f32)), preferred_element_type=f32) * dim ** -0.5
    k = jnp.dot(reach, jnp.abs(wk_ref[...].astype(f32)), preferred_element_type=f32)
    b = jnp.sum(reach[0:1] * jnp.sum(jnp.abs(wb_ref[...].astype(f32)), axis=0, keepdims=True), axis=1, keepdims=True)
    out_ref[...] = jnp.broadcast_to((jnp.sum(q * k, axis=1, keepdims=True) + b) * 1.1, out_ref.shape)


def score_bound(heads, gamma, beta, w_q, w_k, wb_t):
    args = (gamma, beta, w_q, w_k, wb_t)
    return pl.pallas_call(
        functools.partial(bound_kernel, heads),
        in_specs=[whole(x.shape) for x in args],
        out_specs=whole((8, 128)),
        out_shape=jax.ShapeDtypeStruct((8, 128), f32),
        name="bound",
    )(*args)


def norm_kernel(offsets, z_ref, gamma_ref, beta_ref, wb_ref, *out_refs):
    rows, cols, chan = z_ref.shape
    b_ref = out_refs[-1]
    heads = b_ref.shape[1]
    z = z_ref[...].reshape(rows * cols, chan)
    ones = jnp.full((chan, chan), 1.0 / chan, bf16)
    centered = z.astype(f32) - dot(z, ones, NN)
    var = jnp.mean(centered * centered, axis=-1, keepdims=True)
    a = (centered * lax.rsqrt(var + LN_EPS) * gamma_ref[...] + beta_ref[...]).astype(bf16)
    i = pl.program_id(0)
    for out_ref, lo, hi in zip(out_refs, offsets[:-1], offsets[1:]):
        @pl.when((i >= lo) & (i < hi))
        def _():
            out_ref[...] = a.reshape(rows, cols, chan)
    b = dot(wb_ref[...], a, NT)
    for r in range(rows):
        b_ref[r] = b[:heads, r * cols:(r + 1) * cols].astype(bf16)


def normalize(heads, z, gamma, beta, wb_t, start, chunks):
    cols, chan = z.shape[1:]
    step = NORM_ROWS
    first = start // step
    offsets = [sum(chunks[:i]) // step for i in range(len(chunks) + 1)]
    rows = sum(chunks)

    def chunk_spec(lo, hi):
        return pl.BlockSpec((step, cols, chan), lambda i: (jnp.clip(i - lo, 0, hi - lo - 1), 0, 0))

    return pl.pallas_call(
        functools.partial(norm_kernel, offsets),
        grid=(rows // step,),
        in_specs=[
            pl.BlockSpec((step, cols, chan), lambda i: (first + i, 0, 0)),
            whole((1, chan)), whole((1, chan)), whole(wb_t.shape),
        ],
        out_specs=[chunk_spec(lo, hi) for lo, hi in zip(offsets[:-1], offsets[1:])]
        + [pl.BlockSpec((step, heads, cols), lambda i: (i, 0, 0))],
        out_shape=[jax.ShapeDtypeStruct((c, cols, chan), bf16) for c in chunks]
        + [jax.ShapeDtypeStruct((rows, heads, cols), bf16)],
        compiler_params=VMEM_LIMIT,
        cost_estimate=pl.CostEstimate(flops=rows * cols * chan * 300, bytes_accessed=rows * cols * chan * 4, transcendentals=0),
        name="norm",
    )(z, gamma, beta, wb_t)


def bias_kernel(info_ref, *refs):
    parts, out_ref = refs[:-1], refs[-1]
    queries, heads, cols = parts[0].shape
    base, length = info_ref[1], info_ref[2]
    for m, part in enumerate(parts):
        first = pl.multiple_of((base ^ m) * cols, cols)
        key = first + lax.broadcasted_iota(jnp.int32, (cols, queries), 0)
        key_bias = jnp.where(key < length, 0.0, -1e9).astype(f32)
        b = part[...].astype(f32)
        for h in range(heads):
            out_ref[pl.ds(first, cols), h * queries:(h + 1) * queries] = b[:, h, :].T + key_bias


def lay_bias(info, parts):
    queries, heads, cols = parts[0].shape
    shape = (len(parts) * cols, heads * queries)
    return pl.pallas_call(
        bias_kernel,
        grid_spec=pltpu.PrefetchScalarGridSpec(
            num_scalar_prefetch=1, grid=(1,),
            in_specs=[whole(p.shape) for p in parts], out_specs=whole(shape),
        ),
        out_shape=jax.ShapeDtypeStruct(shape, f32),
        compiler_params=VMEM_LIMIT,
        name="bias",
    )(info, *parts)


def attend_kernel(heads, sizes, info_ref, *refs):
    blocks = refs[:4]
    z_ref, bias_ref, wkv_ref, wqg_ref, wo_ref = refs[4:9]
    out_ref, k_s, vt_s, q_s, g_s, s_s, m_s, p_s, l_s, o_s = refs[-10:]
    step, cols, chan = z_ref.shape
    dim = chan // heads
    col, used = info_ref[0], info_ref[3]
    lane_head = lax.broadcasted_iota(jnp.int32, (1, 1, chan), 2) // dim

    for p, ref in enumerate(blocks):
        first = pl.multiple_of((col ^ p) * cols, cols)

        @pl.when(first < used)
        def _():
            kv = dot(ref[...].reshape(step * cols, chan), wkv_ref[...], NN).astype(bf16)
            k_s[:, pl.ds(first, cols), :] = kv[:, :chan].reshape(step, cols, chan)
            v = kv[:, chan:].reshape(step, cols, chan)
            for r in range(step):
                vt_s[r, :, pl.ds(first, cols)] = v[r].T

    qg = dot(blocks[0][...].reshape(step * cols, chan), wqg_ref[...], NN)
    q = (qg[:, :chan] * dim ** -0.5).astype(bf16).reshape(step, cols, chan)
    for h in range(heads):
        q_s[:, h * cols:(h + 1) * cols, :] = jnp.where(lane_head == h, q, jnp.zeros_like(q))
    g_s[...] = jax.nn.sigmoid(qg[:, chan:]).reshape(step, cols, chan)

    def run(keys):
        def score(r, g):
            sl = slice(2 * g * cols, (2 * g + 2) * cols)
            s = dot(k_s[r, :keys, :], q_s[r, sl, :], NT) + bias_ref[:keys, sl]
            s_s[g, :keys, :] = s
            m_s[g] = jnp.max(s, axis=0, keepdims=True)

        def weigh(g):
            p = jnp.exp(s_s[g, :keys, :] - m_s[g])
            l_s[g] = 1.0 / jnp.sum(p, axis=0, keepdims=True)
            p_s[g, :keys, :] = p.astype(bf16)

        def mix(r, g):
            o = dot(vt_s[r, 2 * g * dim:(2 * g + 2) * dim, :keys], p_s[g, :keys, :], NN)
            inv = l_s[g]
            o_s[r, 2 * g * dim:(2 * g + 1) * dim, :] = o[:dim, :cols] * inv[:, :cols]
            o_s[r, (2 * g + 1) * dim:(2 * g + 2) * dim, :] = o[dim:, cols:] * inv[:, cols:]

        score(0, 0)

        def body(r, carry):
            score(r, 1)
            mix(lax.rem(r + step - 1, step), 1)
            weigh(0)
            score(lax.rem(r + 1, step), 0)
            mix(r, 0)
            weigh(1)
            return carry

        lax.fori_loop(0, step, body, 0)
        mix(step - 1, 1)

    for keys in sizes:
        pl.when(used == keys)(functools.partial(run, keys))

    gated = jnp.concatenate([(o_s[r].T * g_s[r]).astype(bf16) for r in range(step)], axis=0)
    update = dot(gated, wo_ref[...], NN)
    out_ref[...] = (z_ref[...].astype(f32) + update.reshape(step, cols, chan)).astype(bf16)


def attend(heads, sizes, info, blocks, z, bias, weights, prev, start, rows):
    cols, chan = z.shape[1:]
    step = ATTEND_ROWS
    first = start // step
    keys, pairs, wide = 4 * cols, heads // 2, 2 * cols
    here = pl.BlockSpec((step, cols, chan), lambda i, _: (i, 0, 0))
    there = pl.BlockSpec((step, cols, chan), lambda i, _: (first + i, 0, 0))
    args = [info] + list(blocks) + [z, bias] + list(weights)
    specs = [here] * 4 + [there, whole(bias.shape)] + [whole(w.shape) for w in weights]
    alias = {}
    if prev is not None:
        alias = {len(args): 0}
        args.append(prev)
        specs.append(pl.BlockSpec(memory_space=pl.ANY))
    return pl.pallas_call(
        functools.partial(attend_kernel, heads, sizes),
        grid_spec=pltpu.PrefetchScalarGridSpec(
            num_scalar_prefetch=1, grid=(rows // step,), in_specs=specs, out_specs=there,
            scratch_shapes=[
                pltpu.VMEM((step, keys, chan), bf16),
                pltpu.VMEM((step, chan, keys), bf16),
                pltpu.VMEM((step, heads * cols, chan), bf16),
                pltpu.VMEM((step, cols, chan), f32),
                pltpu.VMEM((pairs, keys, wide), f32),
                pltpu.VMEM((pairs, 1, wide), f32),
                pltpu.VMEM((pairs, keys, wide), bf16),
                pltpu.VMEM((pairs, 1, wide), f32),
                pltpu.VMEM((step, chan, cols), f32),
            ],
        ),
        out_shape=jax.ShapeDtypeStruct(z.shape, z.dtype),
        input_output_aliases=alias,
        compiler_params=VMEM_LIMIT,
        cost_estimate=pl.CostEstimate(flops=rows * cols * chan * 8000, bytes_accessed=rows * cols * chan * 12, transcendentals=0),
        name="attend",
    )(*args)


def solution(mesh):
    tile_spec = P(('dp', 'row'), 'col', None)
    num_rows, num_cols = mesh.shape['row'], mesh.shape['col']
    x_pairs = [(c, c ^ 2) for c in range(num_cols)]
    core_pairs = [(c, c ^ 1) for c in range(num_cols)]

    def bias_pairs(m):
        pairs = []
        for r in range(num_rows):
            for c in range(num_cols):
                e = c ^ m
                pairs.append((r * num_cols + c, (e >> 1) * num_cols + 2 * r + (e & 1)))
        return pairs

    def inner(z, res_mask, ln_gamma, ln_beta, w_q, w_k, w_v, w_b, w_g, w_o):
        row_len, cols, chan = z.shape
        heads = w_b.shape[1]
        sizes = (2 * cols, 3 * cols, 7 * cols // 2, 4 * cols)
        row_idx, col_idx = lax.axis_index('row'), lax.axis_index('col')
        gamma, beta = ln_gamma.reshape(1, chan), ln_beta.reshape(1, chan)
        wb_t = jnp.pad(w_b.T, ((0, 8 - heads), (0, 0)))
        weights = (jnp.concatenate([w_k, w_v], axis=1), jnp.concatenate([w_q, w_g], axis=1), w_o)

        starts = [sum(CHUNKS[:i]) for i in range(len(CHUNKS))]
        head = normalize(heads, z, gamma, beta, wb_t, 0, CHUNKS[:1])
        tail = normalize(heads, z, gamma, beta, wb_t, CHUNKS[0], CHUNKS[1:])
        own = head[:-1] + tail[:-1]
        halves = jnp.concatenate([head[-1], tail[-1]], axis=0).reshape(2, row_len // 2, heads, cols)

        length = jnp.sum(res_mask)
        bound = score_bound(heads, gamma, beta, w_q, w_k, wb_t)[0, 0]
        used = jnp.where(length <= sizes[0], sizes[0], jnp.where(length <= sizes[1], sizes[1], sizes[2]))
        used = jnp.where(bound < SCORE_BOUND, used, sizes[3])
        info = jnp.stack([col_idx, 2 * row_idx + (col_idx & 1), length, used]).astype(jnp.int32)

        parts = []
        for m in range(4):
            half = lax.dynamic_index_in_dim(halves, (col_idx ^ m) & 1, 0, keepdims=False)
            parts.append(lax.ppermute(half, ('row', 'col'), bias_pairs(m)))
        bias = lay_bias(info, parts)
        far, near = [], []
        for a in own:
            far.append(lax.ppermute(a, 'col', x_pairs))
            near.append(lax.ppermute(a, 'col', core_pairs))
        out = None
        for i, (start, rows) in enumerate(zip(starts, CHUNKS)):
            diag = lax.ppermute(far[i], 'col', core_pairs)
            out = attend(heads, sizes, info, (own[i], near[i], far[i], diag), z, bias, weights, out, start, rows)
        return out

    return jax.shard_map(inner, mesh=mesh, in_specs=(tile_spec, P('dp'), P(), P(), P(), P(), P(), P(), P(), P()), out_specs=tile_spec, check_vma=False)
```

```python
import functools

import jax
import jax.numpy as jnp
from jax import lax
from jax.experimental import pallas as pl
from jax.experimental.pallas import tpu as pltpu
from jax.sharding import PartitionSpec as P


LN_EPS = 1e-5
CHUNKS = (32, 16, 48, 48, 48, 32, 16, 16)
NORM_ROWS = 16
ATTEND_ROWS = 16
SCORE_BOUND = 1e8
VALUE_BOUND = 1e20
SUM_RANGE = (1e-10, 1e15)
NN = (((1,), (0,)), ((), ()))
NT = (((1,), (1,)), ((), ()))
f32, bf16 = jnp.float32, jnp.bfloat16
dot = functools.partial(lax.dot_general, preferred_element_type=f32)
VMEM_LIMIT = pltpu.CompilerParams(vmem_limit_bytes=67043328)


def whole(shape):
    return pl.BlockSpec(shape, lambda *_: (0,) * len(shape))


def bound_kernel(heads, gamma_ref, beta_ref, wq_ref, wk_ref, wv_ref, wb_ref, out_ref):
    chan = gamma_ref.shape[1]
    dim = chan // heads
    reach = jnp.broadcast_to(jnp.abs(gamma_ref[...]) * chan ** 0.5 + jnp.abs(beta_ref[...]), (8, chan)) * 1.05
    q = jnp.dot(reach, jnp.abs(wq_ref[...].astype(f32)), preferred_element_type=f32) * dim ** -0.5
    k = jnp.dot(reach, jnp.abs(wk_ref[...].astype(f32)), preferred_element_type=f32)
    v = jnp.dot(reach, jnp.abs(wv_ref[...].astype(f32)), preferred_element_type=f32)
    b = jnp.sum(reach[0:1] * jnp.sum(jnp.abs(wb_ref[...].astype(f32)), axis=0, keepdims=True), axis=1, keepdims=True)
    s = jnp.sum(q * k, axis=1, keepdims=True) + b
    row = lax.broadcasted_iota(jnp.int32, out_ref.shape, 0)
    out_ref[...] = jnp.where(row == 0, s, jnp.max(v, axis=1, keepdims=True)) * 1.1


def bounds(heads, gamma, beta, w_q, w_k, w_v, wb_t):
    args = (gamma, beta, w_q, w_k, w_v, wb_t)
    return pl.pallas_call(
        functools.partial(bound_kernel, heads),
        in_specs=[whole(x.shape) for x in args],
        out_specs=whole((8, 128)),
        out_shape=jax.ShapeDtypeStruct((8, 128), f32),
        name="bound",
    )(*args)


def norm_kernel(offsets, z_ref, gamma_ref, beta_ref, wb_ref, *out_refs):
    rows, cols, chan = z_ref.shape
    b_ref = out_refs[-1]
    heads = b_ref.shape[1]
    z = z_ref[...].reshape(rows * cols, chan)
    ones = jnp.full((chan, chan), 1.0 / chan, bf16)
    centered = z.astype(f32) - dot(z, ones, NN)
    var = jnp.mean(centered * centered, axis=-1, keepdims=True)
    a = (centered * lax.rsqrt(var + LN_EPS) * gamma_ref[...] + beta_ref[...]).astype(bf16)
    i = pl.program_id(0)
    for out_ref, lo, hi in zip(out_refs, offsets[:-1], offsets[1:]):
        @pl.when((i >= lo) & (i < hi))
        def _():
            out_ref[...] = a.reshape(rows, cols, chan)
    b = dot(wb_ref[...], a, NT)
    for r in range(rows):
        b_ref[r] = b[:heads, r * cols:(r + 1) * cols].astype(bf16)


def normalize(heads, z, gamma, beta, wb_t, start, chunks):
    cols, chan = z.shape[1:]
    step = NORM_ROWS
    first = start // step
    offsets = [sum(chunks[:i]) // step for i in range(len(chunks) + 1)]
    rows = sum(chunks)

    def chunk_spec(lo, hi):
        return pl.BlockSpec((step, cols, chan), lambda i: (jnp.clip(i - lo, 0, hi - lo - 1), 0, 0))

    return pl.pallas_call(
        functools.partial(norm_kernel, offsets),
        grid=(rows // step,),
        in_specs=[
            pl.BlockSpec((step, cols, chan), lambda i: (first + i, 0, 0)),
            whole((1, chan)), whole((1, chan)), whole(wb_t.shape),
        ],
        out_specs=[chunk_spec(lo, hi) for lo, hi in zip(offsets[:-1], offsets[1:])]
        + [pl.BlockSpec((step, heads, cols), lambda i: (i, 0, 0))],
        out_shape=[jax.ShapeDtypeStruct((c, cols, chan), bf16) for c in chunks]
        + [jax.ShapeDtypeStruct((rows, heads, cols), bf16)],
        compiler_params=VMEM_LIMIT,
        cost_estimate=pl.CostEstimate(flops=rows * cols * chan * 300, bytes_accessed=rows * cols * chan * 4, transcendentals=0),
        name="norm",
    )(z, gamma, beta, wb_t)


def bias_kernel(info_ref, *refs):
    parts, out_ref = refs[:-1], refs[-1]
    queries, heads, cols = parts[0].shape
    base, length = info_ref[1], info_ref[2]
    for m, part in enumerate(parts):
        first = pl.multiple_of((base ^ m) * cols, cols)
        key = first + lax.broadcasted_iota(jnp.int32, (cols, queries), 0)
        key_bias = jnp.where(key < length, 0.0, -1e9).astype(f32)
        b = part[...].astype(f32)
        for h in range(heads):
            out_ref[pl.ds(first, cols), h * queries:(h + 1) * queries] = b[:, h, :].T + key_bias


def lay_bias(info, parts):
    queries, heads, cols = parts[0].shape
    shape = (len(parts) * cols, heads * queries)
    return pl.pallas_call(
        bias_kernel,
        grid_spec=pltpu.PrefetchScalarGridSpec(
            num_scalar_prefetch=1, grid=(1,),
            in_specs=[whole(p.shape) for p in parts], out_specs=whole(shape),
        ),
        out_shape=jax.ShapeDtypeStruct(shape, f32),
        compiler_params=VMEM_LIMIT,
        name="bias",
    )(info, *parts)


def attend_kernel(heads, sizes, info_ref, *refs):
    blocks = refs[:4]
    z_ref, bias_ref, wkv_ref, wqg_ref, wo_ref = refs[4:9]
    out_ref, k_s, vt_s, q_s, g_s, p_s, l_s, o_s = refs[-8:]
    step, cols, chan = z_ref.shape
    dim = chan // heads
    col, used = info_ref[0], info_ref[3]

    @pl.when(pl.program_id(0) == 0)
    def _():
        k_s[...] = jnp.zeros_like(k_s)
        vt_s[...] = jnp.zeros_like(vt_s)
        q_s[...] = jnp.zeros_like(q_s)

    for p, ref in enumerate(blocks):
        first = pl.multiple_of((col ^ p) * cols, cols)

        @pl.when(first < used)
        def _():
            kv = dot(ref[...].reshape(step * cols, chan), wkv_ref[...], NN).astype(bf16)
            k_s[:, pl.ds(first, cols), :] = kv[:, :chan].reshape(step, cols, chan)
            v = kv[:, chan:].reshape(step, cols, chan)
            for r in range(step):
                vt_s[r, :, pl.ds(first, cols)] = v[r].T

    qg = dot(blocks[0][...].reshape(step * cols, chan), wqg_ref[...], NN)
    q = (qg[:, :chan] * dim ** -0.5).astype(bf16).reshape(step, cols, chan)
    for r in range(step):
        q_t = q[r].T
        for h in range(heads):
            q_s[r, h * dim:(h + 1) * dim, h * cols:(h + 1) * cols] = q_t[h * dim:(h + 1) * dim]
    g_s[...] = jax.nn.sigmoid(qg[:, chan:]).reshape(step, cols, chan)

    def run(keys, shift):
        def weigh(r, slot):
            s = dot(k_s[r, :keys, :], q_s[r], NN) + bias_ref[:keys, :]
            e = jnp.exp(s - jnp.max(s, axis=0, keepdims=True) if shift else s)
            l_s[r] = jnp.sum(e, axis=0, keepdims=True)
            p_s[slot, :keys, :] = e.astype(bf16)

        def mix(r, slot):
            o = dot(vt_s[r, :, :keys], p_s[slot, :keys, :], NN)
            inv = 1.0 / l_s[r]
            for h in range(heads):
                part = o[h * dim:(h + 1) * dim, h * cols:(h + 1) * cols]
                o_s[r, h * dim:(h + 1) * dim, :] = part * inv[:, h * cols:(h + 1) * cols]

        def pair(i, carry):
            r = 2 * i
            weigh(r, 0)
            mix(lax.rem(r + step - 1, step), 1)
            weigh(r + 1, 1)
            mix(r, 0)
            return carry

        def single(r, carry):
            weigh(r, 0)
            mix(r, 0)
            return carry

        if shift:
            lax.fori_loop(0, step, single, 0)
        else:
            lax.fori_loop(0, step // 2, pair, 0)
            mix(step - 1, 1)

    for keys in sizes[:-1]:
        pl.when(used == keys)(functools.partial(run, keys, False))
    l = l_s[...]
    fine = (used < sizes[-1]) & (jnp.min(l) > SUM_RANGE[0]) & (jnp.max(l) < SUM_RANGE[1])
    pl.when(jnp.logical_not(fine))(functools.partial(run, sizes[-1], True))

    gated = jnp.concatenate([(o_s[r].T * g_s[r]).astype(bf16) for r in range(step)], axis=0)
    update = dot(gated, wo_ref[...], NN)
    out_ref[...] = (z_ref[...].astype(f32) + update.reshape(step, cols, chan)).astype(bf16)


def attend(heads, sizes, info, blocks, z, bias, weights, prev, start, rows):
    cols, chan = z.shape[1:]
    step = ATTEND_ROWS
    first = start // step
    keys = 4 * cols
    here = pl.BlockSpec((step, cols, chan), lambda i, _: (i, 0, 0))
    there = pl.BlockSpec((step, cols, chan), lambda i, _: (first + i, 0, 0))
    args = [info] + list(blocks) + [z, bias] + list(weights)
    specs = [here] * 4 + [there, whole(bias.shape)] + [whole(w.shape) for w in weights]
    alias = {}
    if prev is not None:
        alias = {len(args): 0}
        args.append(prev)
        specs.append(pl.BlockSpec(memory_space=pl.ANY))
    return pl.pallas_call(
        functools.partial(attend_kernel, heads, sizes),
        grid_spec=pltpu.PrefetchScalarGridSpec(
            num_scalar_prefetch=1, grid=(rows // step,), in_specs=specs, out_specs=there,
            scratch_shapes=[
                pltpu.VMEM((step, keys, chan), bf16),
                pltpu.VMEM((step, chan, keys), bf16),
                pltpu.VMEM((step, chan, heads * cols), bf16),
                pltpu.VMEM((step, cols, chan), f32),
                pltpu.VMEM((2, keys, heads * cols), bf16),
                pltpu.VMEM((step, 1, heads * cols), f32),
                pltpu.VMEM((step, chan, cols), f32),
            ],
        ),
        out_shape=jax.ShapeDtypeStruct(z.shape, z.dtype),
        input_output_aliases=alias,
        compiler_params=VMEM_LIMIT,
        cost_estimate=pl.CostEstimate(flops=rows * cols * chan * 8000, bytes_accessed=rows * cols * chan * 12, transcendentals=0),
        name="attend",
    )(*args)


def solution(mesh):
    tile_spec = P(('dp', 'row'), 'col', None)
    num_rows, num_cols = mesh.shape['row'], mesh.shape['col']
    x_pairs = [(c, c ^ 2) for c in range(num_cols)]
    core_pairs = [(c, c ^ 1) for c in range(num_cols)]

    def bias_pairs(m):
        pairs = []
        for r in range(num_rows):
            for c in range(num_cols):
                e = c ^ m
                pairs.append((r * num_cols + c, (e >> 1) * num_cols + 2 * r + (e & 1)))
        return pairs

    def inner(z, res_mask, ln_gamma, ln_beta, w_q, w_k, w_v, w_b, w_g, w_o):
        row_len, cols, chan = z.shape
        heads = w_b.shape[1]
        sizes = (2 * cols, 3 * cols, 7 * cols // 2, 4 * cols)
        row_idx, col_idx = lax.axis_index('row'), lax.axis_index('col')
        gamma, beta = ln_gamma.reshape(1, chan), ln_beta.reshape(1, chan)
        wb_t = jnp.pad(w_b.T, ((0, 8 - heads), (0, 0)))
        weights = (jnp.concatenate([w_k, w_v], axis=1), jnp.concatenate([w_q, w_g], axis=1), w_o)

        starts = [sum(CHUNKS[:i]) for i in range(len(CHUNKS))]
        head = normalize(heads, z, gamma, beta, wb_t, 0, CHUNKS[:1])
        tail = normalize(heads, z, gamma, beta, wb_t, CHUNKS[0], CHUNKS[1:])
        own = head[:-1] + tail[:-1]
        halves = jnp.concatenate([head[-1], tail[-1]], axis=0).reshape(2, row_len // 2, heads, cols)

        length = jnp.sum(res_mask)
        bound = bounds(heads, gamma, beta, w_q, w_k, w_v, wb_t)
        used = jnp.where(length <= sizes[0], sizes[0], jnp.where(length <= sizes[1], sizes[1], sizes[2]))
        used = jnp.where((bound[0, 0] < SCORE_BOUND) & (bound[1, 0] < VALUE_BOUND), used, sizes[3])
        info = jnp.stack([col_idx, 2 * row_idx + (col_idx & 1), length, used]).astype(jnp.int32)

        parts = []
        for m in range(4):
            half = lax.dynamic_index_in_dim(halves, (col_idx ^ m) & 1, 0, keepdims=False)
            parts.append(lax.ppermute(half, ('row', 'col'), bias_pairs(m)))
        bias = lay_bias(info, parts)
        far, near = [], []
        for a in own:
            far.append(lax.ppermute(a, 'col', x_pairs))
            near.append(lax.ppermute(a, 'col', core_pairs))
        out = None
        for i, (start, rows) in enumerate(zip(starts, CHUNKS)):
            diag = lax.ppermute(far[i], 'col', core_pairs)
            out = attend(heads, sizes, info, (own[i], near[i], far[i], diag), z, bias, weights, out, start, rows)
        return out

    return jax.shard_map(inner, mesh=mesh, in_specs=(tile_spec, P('dp'), P(), P(), P(), P(), P(), P(), P(), P()), out_specs=tile_spec, check_vma=False)
```

```python
import functools

import jax
import jax.numpy as jnp
from jax import lax
from jax.experimental import pallas as pl
from jax.experimental.pallas import tpu as pltpu
from jax.sharding import PartitionSpec as P


LN_EPS = 1e-5
CHUNKS = (32, 64, 32, 32, 32, 32, 16, 16)
NORM_ROWS = 32
ATTEND_ROWS = 16
GROUP = 8
SCORE_BOUND = 1e8
VALUE_BOUND = 1e20
SUM_RANGE = (1e-10, 1e15)
NN = (((1,), (0,)), ((), ()))
NT = (((1,), (1,)), ((), ()))
f32, bf16 = jnp.float32, jnp.bfloat16
dot = functools.partial(lax.dot_general, preferred_element_type=f32)
VMEM_LIMIT = pltpu.CompilerParams(vmem_limit_bytes=67043328)


def whole(shape):
    return pl.BlockSpec(shape, lambda *_: (0,) * len(shape))


def plan_kernel(heads, sizes, mask_ref, gamma_ref, beta_ref, wq_ref, wk_ref, wv_ref, wb_ref, wg_ref, info_ref, wkv_ref, wqg_ref):
    chan = gamma_ref.shape[1]
    dim = chan // heads
    row_idx, col_idx = lax.axis_index('row'), lax.axis_index('col')
    wkv_ref[:, :chan], wkv_ref[:, chan:] = wk_ref[...], wv_ref[...]
    wqg_ref[:, :chan], wqg_ref[:, chan:] = wq_ref[...], wg_ref[...]
    reach = jnp.broadcast_to(jnp.abs(gamma_ref[...]) * chan ** 0.5 + jnp.abs(beta_ref[...]), (8, chan)) * 1.05
    q = jnp.dot(reach, jnp.abs(wq_ref[...].astype(f32)), preferred_element_type=f32) * dim ** -0.5
    k = jnp.dot(reach, jnp.abs(wk_ref[...].astype(f32)), preferred_element_type=f32)
    v = jnp.dot(reach, jnp.abs(wv_ref[...].astype(f32)), preferred_element_type=f32)
    b = jnp.dot(reach, jnp.abs(wb_ref[...].astype(f32)), preferred_element_type=f32)
    s_bound = (jnp.sum(q * k) + jnp.sum(b)) * 1.1
    v_bound = jnp.max(v) * 1.1
    length = jnp.sum(mask_ref[...].astype(f32)).astype(jnp.int32)
    used = jnp.where(length <= sizes[0], sizes[0], sizes[1])
    info_ref[0] = col_idx
    info_ref[1] = 2 * row_idx + (col_idx & 1)
    info_ref[2] = length
    info_ref[3] = jnp.where((s_bound < SCORE_BOUND) & (v_bound < VALUE_BOUND), used, sizes[2])


def make_plan(heads, sizes, *args):
    chan = args[1].shape[1]
    return pl.pallas_call(
        functools.partial(plan_kernel, heads, sizes),
        in_specs=[whole(x.shape) for x in args],
        out_specs=[pl.BlockSpec(memory_space=pltpu.SMEM), whole((chan, 2 * chan)), whole((chan, 2 * chan))],
        out_shape=[jax.ShapeDtypeStruct((4,), jnp.int32)] + [jax.ShapeDtypeStruct((chan, 2 * chan), bf16)] * 2,
        compiler_params=VMEM_LIMIT,
        name="plan",
    )(*args)


def norm_kernel(places, z_ref, gamma_ref, beta_ref, wb_ref, *out_refs):
    rows, cols, chan = z_ref.shape
    b_ref = out_refs[len(places)]
    heads = b_ref.shape[1]
    z = z_ref[...].reshape(rows * cols, chan)
    ones = jnp.full((chan, chan), 1.0 / chan, bf16)
    centered = z.astype(f32) - dot(z, ones, NN)
    var = jnp.mean(centered * centered, axis=-1, keepdims=True)
    a = (centered * lax.rsqrt(var + LN_EPS) * gamma_ref[...] + beta_ref[...]).astype(bf16)
    blocks = a.reshape(rows, cols, chan)
    i = pl.program_id(0)
    for out_ref, (lo, steps, offset) in zip(out_refs, places):
        @pl.when((i >= lo) & (i < lo + steps))
        def _():
            out_ref[...] = blocks[offset:offset + out_ref.shape[0]]
    for out_ref in out_refs[len(places) + 1:]:
        out_ref[...] = blocks
    wb = jnp.concatenate([wb_ref[...].astype(f32), jnp.zeros((chan, chan - heads), f32)], axis=1).T[:8].astype(bf16)
    b = dot(wb, a, NT)
    for r in range(rows):
        b_ref[r] = b[:heads, r * cols:(r + 1) * cols].astype(bf16)


def normalize(z, gamma, beta, w_b, start, chunks, joined):
    cols, chan = z.shape[1:]
    heads = w_b.shape[1]
    step = NORM_ROWS
    first = start // step
    rows = sum(chunks)
    places, specs = [], []
    for i, c in enumerate(chunks):
        lo, offset = divmod(sum(chunks[:i]), step)
        steps = max(c // step, 1)
        places.append((lo, steps, offset))
        specs.append(pl.BlockSpec((min(step, c), cols, chan), lambda i, lo=lo, steps=steps: (jnp.clip(i - lo, 0, steps - 1), 0, 0)))
    specs.append(pl.BlockSpec((step, heads, cols), lambda i: (i, 0, 0)))
    shapes = [jax.ShapeDtypeStruct((c, cols, chan), bf16) for c in chunks] + [jax.ShapeDtypeStruct((rows, heads, cols), bf16)]
    if joined:
        specs.append(pl.BlockSpec((step, cols, chan), lambda i: (i, 0, 0)))
        shapes.append(jax.ShapeDtypeStruct((rows, cols, chan), bf16))
    return pl.pallas_call(
        functools.partial(norm_kernel, places),
        grid=(rows // step,),
        in_specs=[
            pl.BlockSpec((step, cols, chan), lambda i: (first + i, 0, 0)),
            whole((1, chan)), whole((1, chan)), whole(w_b.shape),
        ],
        out_specs=specs,
        out_shape=shapes,
        compiler_params=VMEM_LIMIT,
        cost_estimate=pl.CostEstimate(flops=rows * cols * chan * 300, bytes_accessed=rows * cols * chan * 4, transcendentals=0),
        name="norm",
    )(z, gamma, beta, w_b)


def bias_kernel(info_ref, *refs):
    parts, out_ref = refs[:-1], refs[-1]
    queries, heads, cols = parts[0].shape
    base, length = info_ref[1], info_ref[2]
    for m, part in enumerate(parts):
        first = pl.multiple_of((base ^ m) * cols, cols)
        key = first + lax.broadcasted_iota(jnp.int32, (cols, queries), 0)
        key_bias = jnp.where(key < length, 0.0, -1e9).astype(f32)
        b = part[...].astype(f32)
        for h in range(heads):
            out_ref[pl.ds(first, cols), h * queries:(h + 1) * queries] = b[:, h, :].T + key_bias


def lay_bias(info, parts):
    queries, heads, cols = parts[0].shape
    shape = (len(parts) * cols, heads * queries)
    return pl.pallas_call(
        bias_kernel,
        grid_spec=pltpu.PrefetchScalarGridSpec(
            num_scalar_prefetch=1, grid=(1,),
            in_specs=[whole(p.shape) for p in parts], out_specs=whole(shape),
        ),
        out_shape=jax.ShapeDtypeStruct(shape, f32),
        compiler_params=VMEM_LIMIT,
        name="bias",
    )(info, *parts)


def attend_kernel(heads, sizes, info_ref, *refs):
    blocks = refs[:4]
    z_ref, bias_ref, wkv_ref, wqg_ref, wo_ref = refs[4:9]
    out_ref, k_s, vt_s, q_s, g_s, p_s, l_s, o_s = refs[-8:]
    step, cols, chan = z_ref.shape
    dim = chan // heads
    col, used = info_ref[0], info_ref[3]

    @pl.when(pl.program_id(0) == 0)
    def _():
        q_s[...] = jnp.zeros_like(q_s)

    def project(i, carry):
        rows = pl.ds(GROUP * i, GROUP)
        for p, ref in enumerate(blocks):
            first = pl.multiple_of((col ^ p) * cols, cols)
            kv = dot(ref[rows].reshape(GROUP * cols, chan), wkv_ref[...], NN).astype(bf16)
            k_s[rows, pl.ds(first, cols), :] = kv[:, :chan].reshape(GROUP, cols, chan)
            v = kv[:, chan:].reshape(GROUP, cols, chan)
            for r in range(GROUP):
                vt_s[GROUP * i + r, :, pl.ds(first, cols)] = v[r].T
        qg = dot(blocks[0][rows].reshape(GROUP * cols, chan), wqg_ref[...], NN)
        q = (qg[:, :chan] * dim ** -0.5).astype(bf16).reshape(GROUP, cols, chan)
        for r in range(GROUP):
            q_t = q[r].T
            for h in range(heads):
                q_s[GROUP * i + r, h * dim:(h + 1) * dim, h * cols:(h + 1) * cols] = q_t[h * dim:(h + 1) * dim]
        g_s[rows] = jax.nn.sigmoid(qg[:, chan:]).reshape(GROUP, cols, chan)
        return carry

    lax.fori_loop(0, step // GROUP, project, 0)

    def run(keys, shift):
        def weigh(r, slot):
            s = dot(k_s[r, :keys, :], q_s[r], NN) + bias_ref[:keys, :]
            e = jnp.exp(s - jnp.max(s, axis=0, keepdims=True) if shift else s)
            l_s[r] = jnp.sum(e, axis=0, keepdims=True)
            p_s[slot, :keys, :] = e.astype(bf16)

        def mix(r, slot):
            o = dot(vt_s[r, :, :keys], p_s[slot, :keys, :], NN)
            inv = 1.0 / l_s[r]
            for h in range(heads):
                part = o[h * dim:(h + 1) * dim, h * cols:(h + 1) * cols]
                o_s[r, h * dim:(h + 1) * dim, :] = part * inv[:, h * cols:(h + 1) * cols]

        def pair(i, carry):
            r = 2 * i
            weigh(r, 0)
            mix(lax.rem(r + step - 1, step), 1)
            weigh(r + 1, 1)
            mix(r, 0)
            return carry

        def single(r, carry):
            weigh(r, 0)
            mix(r, 0)
            return carry

        if shift:
            lax.fori_loop(0, step, single, 0)
        else:
            lax.fori_loop(0, step // 2, pair, 0)
            mix(step - 1, 1)

    for keys in sizes[:-1]:
        pl.when(used == keys)(functools.partial(run, keys, False))
    l = l_s[...]
    fine = (used < sizes[-1]) & (jnp.min(l) > SUM_RANGE[0]) & (jnp.max(l) < SUM_RANGE[1])
    pl.when(jnp.logical_not(fine))(functools.partial(run, sizes[-1], True))

    def finish(i, carry):
        rows = pl.ds(GROUP * i, GROUP)
        gated = jnp.concatenate([(o_s[GROUP * i + r].T * g_s[GROUP * i + r]).astype(bf16) for r in range(GROUP)], axis=0)
        update = dot(gated, wo_ref[...], NN).reshape(GROUP, cols, chan)
        out_ref[rows] = (z_ref[rows].astype(f32) + update).astype(bf16)
        return carry

    lax.fori_loop(0, step // GROUP, finish, 0)


def attend(heads, sizes, info, blocks, skips, z, bias, weights, prev, start, rows):
    cols, chan = z.shape[1:]
    step = ATTEND_ROWS
    first = start // step
    keys = 4 * cols
    here = [pl.BlockSpec((step, cols, chan), lambda i, _, skip=skip: (skip // step + i, 0, 0)) for skip in skips]
    there = pl.BlockSpec((step, cols, chan), lambda i, _: (first + i, 0, 0))
    args = [info] + list(blocks) + [z, bias] + list(weights)
    specs = here + [there, whole(bias.shape)] + [whole(w.shape) for w in weights]
    alias = {}
    if prev is not None:
        alias = {len(args): 0}
        args.append(prev)
        specs.append(pl.BlockSpec(memory_space=pl.ANY))
    return pl.pallas_call(
        functools.partial(attend_kernel, heads, sizes),
        grid_spec=pltpu.PrefetchScalarGridSpec(
            num_scalar_prefetch=1, grid=(rows // step,), in_specs=specs, out_specs=there,
            scratch_shapes=[
                pltpu.VMEM((step, keys, chan), bf16),
                pltpu.VMEM((step, chan, keys), bf16),
                pltpu.VMEM((step, chan, heads * cols), bf16),
                pltpu.VMEM((step, cols, chan), f32),
                pltpu.VMEM((2, keys, heads * cols), bf16),
                pltpu.VMEM((step, 1, heads * cols), f32),
                pltpu.VMEM((step, chan, cols), f32),
            ],
        ),
        out_shape=jax.ShapeDtypeStruct(z.shape, z.dtype),
        input_output_aliases=alias,
        compiler_params=VMEM_LIMIT,
        cost_estimate=pl.CostEstimate(flops=rows * cols * chan * 8000, bytes_accessed=rows * cols * chan * 12, transcendentals=0),
        name="attend",
    )(*args)


def solution(mesh):
    tile_spec = P(('dp', 'row'), 'col', None)
    num_rows, num_cols = mesh.shape['row'], mesh.shape['col']
    x_pairs = [(c, c ^ 2) for c in range(num_cols)]
    core_pairs = [(c, c ^ 1) for c in range(num_cols)]

    def bias_pairs(m):
        pairs = []
        for r in range(num_rows):
            for c in range(num_cols):
                e = c ^ m
                pairs.append((r * num_cols + c, (e >> 1) * num_cols + 2 * r + (e & 1)))
        return pairs

    def inner(z, res_mask, ln_gamma, ln_beta, w_q, w_k, w_v, w_b, w_g, w_o):
        row_len, cols, chan = z.shape
        heads = w_b.shape[1]
        sizes = (3 * cols, 7 * cols // 2, 4 * cols)
        col_idx = lax.axis_index('col')
        gamma, beta = ln_gamma.reshape(1, chan), ln_beta.reshape(1, chan)
        starts = [sum(CHUNKS[:i]) for i in range(len(CHUNKS))]
        head = normalize(z, gamma, beta, w_b, 0, CHUNKS[:1], False)
        *tail, tail_bias, rest = normalize(z, gamma, beta, w_b, CHUNKS[0], CHUNKS[1:], True)
        own = [head[0]] + tail
        halves = jnp.concatenate([head[1], tail_bias], axis=0).reshape(2, row_len // 2, heads, cols)
        info, w_kv, w_qg = make_plan(heads, sizes, res_mask.reshape(4, cols), gamma, beta, w_q, w_k, w_v, w_b, w_g)
        weights = (w_kv, w_qg, w_o)

        parts = []
        for m in range(4):
            half = lax.dynamic_index_in_dim(halves, (col_idx ^ m) & 1, 0, keepdims=False)
            parts.append(lax.ppermute(half, ('row', 'col'), bias_pairs(m)))
        bias = lay_bias(info, parts)
        far, near = [], []
        for a in own:
            far.append(lax.ppermute(a, 'col', x_pairs))
        for a in (own[0], rest):
            near.append(lax.ppermute(a, 'col', core_pairs))
        out = None
        for i, (start, rows) in enumerate(zip(starts, CHUNKS)):
            diag = lax.ppermute(far[i], 'col', core_pairs)
            out = attend(heads, sizes, info, (own[i], near[min(i, 1)], far[i], diag), (0, start - CHUNKS[0] if i else 0, 0, 0), z, bias, weights, out, start, rows)
        return out

    return jax.shard_map(inner, mesh=mesh, in_specs=(tile_spec, P('dp'), P(), P(), P(), P(), P(), P(), P(), P()), out_specs=tile_spec, check_vma=False)
```

```python
import functools

import jax
import jax.numpy as jnp
from jax import lax
from jax.experimental import pallas as pl
from jax.experimental.pallas import tpu as pltpu
from jax.sharding import PartitionSpec as P


LN_EPS = 1e-5
CHUNKS = (16, 48, 48, 48, 32, 32, 32)
NORM_ROWS = 16
ATTEND_ROWS = 16
GROUP = 16
ATTEND_VMEM = (57 * 1024 * 1024, 40 * 1024 * 1024)
SMALL_VMEM = pltpu.CompilerParams(vmem_limit_bytes=24 * 1024 * 1024)
SCORE_BOUND = 1e8
VALUE_BOUND = 1e20
SUM_RANGE = (1e-10, 1e15)
NN = (((1,), (0,)), ((), ()))
NT = (((1,), (1,)), ((), ()))
f32, bf16 = jnp.float32, jnp.bfloat16
dot = functools.partial(lax.dot_general, preferred_element_type=f32)
VMEM_LIMIT = pltpu.CompilerParams(vmem_limit_bytes=67043328)


def whole(shape):
    return pl.BlockSpec(shape, lambda *_: (0,) * len(shape))


def plan_kernel(heads, sizes, mask_ref, gamma_ref, beta_ref, wq_ref, wk_ref, wv_ref, wb_ref, wg_ref, info_ref, wkv_ref, wqg_ref):
    chan = gamma_ref.shape[1]
    dim = chan // heads
    row_idx, col_idx = lax.axis_index('row'), lax.axis_index('col')
    wkv_ref[:, :chan], wkv_ref[:, chan:] = wk_ref[...], wv_ref[...]
    wqg_ref[:, :chan], wqg_ref[:, chan:] = wq_ref[...], wg_ref[...]
    reach = jnp.broadcast_to(jnp.abs(gamma_ref[...]) * chan ** 0.5 + jnp.abs(beta_ref[...]), (8, chan)) * 1.05
    q = jnp.dot(reach, jnp.abs(wq_ref[...].astype(f32)), preferred_element_type=f32) * dim ** -0.5
    k = jnp.dot(reach, jnp.abs(wk_ref[...].astype(f32)), preferred_element_type=f32)
    v = jnp.dot(reach, jnp.abs(wv_ref[...].astype(f32)), preferred_element_type=f32)
    b = reach[:1] * jnp.sum(jnp.abs(wb_ref[...].astype(f32)), axis=0, keepdims=True)
    s_bound = (jnp.sum(q * k) + jnp.sum(b)) * 1.1
    v_bound = jnp.max(v) * 1.1
    length = jnp.sum(mask_ref[...].astype(f32)).astype(jnp.int32)
    used = jnp.where(length <= sizes[0], sizes[0], sizes[1])
    info_ref[0] = col_idx
    info_ref[1] = 2 * row_idx + (col_idx & 1)
    info_ref[2] = length
    info_ref[3] = jnp.where((s_bound < SCORE_BOUND) & (v_bound < VALUE_BOUND), used, sizes[2])


def make_plan(heads, sizes, *args):
    chan = args[1].shape[1]
    return pl.pallas_call(
        functools.partial(plan_kernel, heads, sizes),
        in_specs=[whole(x.shape) for x in args],
        out_specs=[pl.BlockSpec(memory_space=pltpu.SMEM), whole((chan, 2 * chan)), whole((chan, 2 * chan))],
        out_shape=[jax.ShapeDtypeStruct((4,), jnp.int32)] + [jax.ShapeDtypeStruct((chan, 2 * chan), bf16)] * 2,
        compiler_params=SMALL_VMEM,
        name="plan",
    )(*args)


def norm_kernel(places, z_ref, gamma_ref, beta_ref, wb_ref, *out_refs):
    rows, cols, chan = z_ref.shape
    b_ref = out_refs[len(places)]
    z = z_ref[...].reshape(rows * cols, chan)
    ones = jnp.full((chan, chan), 1.0 / chan, bf16)
    centered = z.astype(f32) - dot(z, ones, NN)
    var = jnp.mean(centered * centered, axis=-1, keepdims=True)
    a = (centered * lax.rsqrt(var + LN_EPS) * gamma_ref[...] + beta_ref[...]).astype(bf16)
    blocks = a.reshape(rows, cols, chan)
    i = pl.program_id(0)
    for out_ref, (lo, steps, offset) in zip(out_refs, places):
        @pl.when((i >= lo) & (i < lo + steps))
        def _():
            out_ref[...] = blocks[offset:offset + out_ref.shape[0]]
    for out_ref in out_refs[len(places) + 1:]:
        out_ref[...] = blocks
    b = dot(wb_ref[...], a, NT)
    for r in range(rows):
        b_ref[r] = b[:, r * cols:(r + 1) * cols].astype(bf16)


def normalize(z, gamma, beta, wb_t, start, chunks, joined):
    cols, chan = z.shape[1:]
    heads = wb_t.shape[0]
    step = NORM_ROWS
    first = start // step
    rows = sum(chunks)
    places, specs = [], []
    for i, c in enumerate(chunks):
        lo, offset = divmod(sum(chunks[:i]), step)
        steps = max(c // step, 1)
        places.append((lo, steps, offset))
        specs.append(pl.BlockSpec((min(step, c), cols, chan), lambda i, lo=lo, steps=steps: (jnp.clip(i - lo, 0, steps - 1), 0, 0)))
    specs.append(pl.BlockSpec((step, heads, cols), lambda i: (i, 0, 0)))
    shapes = [jax.ShapeDtypeStruct((c, cols, chan), bf16) for c in chunks] + [jax.ShapeDtypeStruct((rows, heads, cols), bf16)]
    if joined:
        specs.append(pl.BlockSpec((step, cols, chan), lambda i: (i, 0, 0)))
        shapes.append(jax.ShapeDtypeStruct((rows, cols, chan), bf16))
    return pl.pallas_call(
        functools.partial(norm_kernel, places),
        grid=(rows // step,),
        in_specs=[
            pl.BlockSpec((step, cols, chan), lambda i: (first + i, 0, 0)),
            whole((1, chan)), whole((1, chan)), whole(wb_t.shape),
        ],
        out_specs=specs,
        out_shape=shapes,
        compiler_params=VMEM_LIMIT,
        cost_estimate=pl.CostEstimate(flops=rows * cols * chan * 300, bytes_accessed=rows * cols * chan * 4, transcendentals=0),
        name="norm",
    )(z, gamma, beta, wb_t)


def bias_kernel(info_ref, *refs):
    parts, out_ref = refs[:-1], refs[-1]
    queries, heads, cols = parts[0].shape
    base, length = info_ref[1], info_ref[2]
    for m, part in enumerate(parts):
        first = pl.multiple_of((base ^ m) * cols, cols)
        key = first + lax.broadcasted_iota(jnp.int32, (cols, queries), 0)
        key_bias = jnp.where(key < length, 0.0, -1e9).astype(f32)
        b = part[...].astype(f32)
        for h in range(heads):
            out_ref[pl.ds(first, cols), h * queries:(h + 1) * queries] = b[:, h, :].T + key_bias


def lay_bias(info, parts):
    queries, heads, cols = parts[0].shape
    shape = (len(parts) * cols, heads * queries)
    return pl.pallas_call(
        bias_kernel,
        grid_spec=pltpu.PrefetchScalarGridSpec(
            num_scalar_prefetch=1, grid=(1,),
            in_specs=[whole(p.shape) for p in parts], out_specs=whole(shape),
        ),
        out_shape=jax.ShapeDtypeStruct(shape, f32),
        compiler_params=SMALL_VMEM,
        name="bias",
    )(info, *parts)


def attend_kernel(heads, sizes, info_ref, *refs):
    blocks = refs[:4]
    z_ref, bias_ref, wkv_ref, wqg_ref, wo_ref = refs[4:9]
    out_ref, k_s, vt_s, q_s, g_s, p_s, l_s, o_s = refs[-8:]
    step, cols, chan = z_ref.shape
    dim = chan // heads
    col, used = info_ref[0], info_ref[3]

    @pl.when(pl.program_id(0) == 0)
    def _():
        q_s[...] = jnp.zeros_like(q_s)

    def project(i, carry):
        rows = pl.ds(GROUP * i, GROUP)
        for p, ref in enumerate(blocks):
            first = pl.multiple_of((col ^ p) * cols, cols)
            kv = dot(ref[rows].reshape(GROUP * cols, chan), wkv_ref[...], NN).astype(bf16)
            k_s[rows, pl.ds(first, cols), :] = kv[:, :chan].reshape(GROUP, cols, chan)
            v = kv[:, chan:].reshape(GROUP, cols, chan)
            for r in range(GROUP):
                vt_s[GROUP * i + r, :, pl.ds(first, cols)] = v[r].T
        qg = dot(blocks[0][rows].reshape(GROUP * cols, chan), wqg_ref[...], NN)
        q = (qg[:, :chan] * dim ** -0.5).astype(bf16).reshape(GROUP, cols, chan)
        for r in range(GROUP):
            q_t = q[r].T
            for h in range(heads):
                q_s[GROUP * i + r, h * dim:(h + 1) * dim, h * cols:(h + 1) * cols] = q_t[h * dim:(h + 1) * dim]
        g_s[rows] = jax.nn.sigmoid(qg[:, chan:]).reshape(GROUP, cols, chan)
        return carry

    lax.fori_loop(0, step // GROUP, project, 0)

    def run(keys, shift):
        def weigh(r, slot):
            s = dot(k_s[r, :keys, :], q_s[r], NN) + bias_ref[:keys, :]
            e = jnp.exp(s - jnp.max(s, axis=0, keepdims=True) if shift else s)
            l_s[r] = jnp.sum(e, axis=0, keepdims=True)
            p_s[slot, :keys, :] = e.astype(bf16)

        def mix(r, slot):
            o = dot(vt_s[r, :, :keys], p_s[slot, :keys, :], NN)
            inv = 1.0 / l_s[r]
            for h in range(heads):
                part = o[h * dim:(h + 1) * dim, h * cols:(h + 1) * cols]
                o_s[r, h * dim:(h + 1) * dim, :] = part * inv[:, h * cols:(h + 1) * cols]

        def pair(i, carry):
            r = 2 * i
            weigh(r, 0)
            mix(lax.rem(r + step - 1, step), 1)
            weigh(r + 1, 1)
            mix(r, 0)
            return carry

        def single(r, carry):
            weigh(r, 0)
            mix(r, 0)
            return carry

        if shift:
            lax.fori_loop(0, step, single, 0)
        else:
            lax.fori_loop(0, step // 2, pair, 0)
            mix(step - 1, 1)

    for keys in sizes[:-1]:
        pl.when(used == keys)(functools.partial(run, keys, False))
    l = l_s[...]
    fine = (used < sizes[-1]) & (jnp.min(l) > SUM_RANGE[0]) & (jnp.max(l) < SUM_RANGE[1])
    pl.when(jnp.logical_not(fine))(functools.partial(run, sizes[-1], True))

    def finish(i, carry):
        rows = pl.ds(GROUP * i, GROUP)
        gated = jnp.concatenate([(o_s[GROUP * i + r].T * g_s[GROUP * i + r]).astype(bf16) for r in range(GROUP)], axis=0)
        update = dot(gated, wo_ref[...], NN).reshape(GROUP, cols, chan)
        out_ref[rows] = (z_ref[rows].astype(f32) + update).astype(bf16)
        return carry

    lax.fori_loop(0, step // GROUP, finish, 0)


def attend(heads, sizes, info, blocks, skips, z, bias, weights, prev, start, rows):
    cols, chan = z.shape[1:]
    step = ATTEND_ROWS
    first = start // step
    keys = 4 * cols
    here = [pl.BlockSpec((step, cols, chan), lambda i, _, skip=skip: (skip // step + i, 0, 0)) for skip in skips]
    there = pl.BlockSpec((step, cols, chan), lambda i, _: (first + i, 0, 0))
    args = [info] + list(blocks) + [z, bias] + list(weights)
    specs = here + [there, whole(bias.shape)] + [whole(w.shape) for w in weights]
    alias = {}
    if prev is not None:
        alias = {len(args): 0}
        args.append(prev)
        specs.append(pl.BlockSpec(memory_space=pl.ANY))
    return pl.pallas_call(
        functools.partial(attend_kernel, heads, sizes),
        grid_spec=pltpu.PrefetchScalarGridSpec(
            num_scalar_prefetch=1, grid=(rows // step,), in_specs=specs, out_specs=there,
            scratch_shapes=[
                pltpu.VMEM((step, keys, chan), bf16),
                pltpu.VMEM((step, chan, keys), bf16),
                pltpu.VMEM((step, chan, heads * cols), bf16),
                pltpu.VMEM((step, cols, chan), f32),
                pltpu.VMEM((2, keys, heads * cols), bf16),
                pltpu.VMEM((step, 1, heads * cols), f32),
                pltpu.VMEM((step, chan, cols), f32),
            ],
        ),
        out_shape=jax.ShapeDtypeStruct(z.shape, z.dtype),
        input_output_aliases=alias,
        compiler_params=pltpu.CompilerParams(vmem_limit_bytes=ATTEND_VMEM[prev is not None]),
        cost_estimate=pl.CostEstimate(flops=rows * cols * chan * 8000, bytes_accessed=rows * cols * chan * 12, transcendentals=0),
        name="attend",
    )(*args)


def solution(mesh):
    tile_spec = P(('dp', 'row'), 'col', None)
    num_rows, num_cols = mesh.shape['row'], mesh.shape['col']
    x_pairs = [(c, c ^ 2) for c in range(num_cols)]
    core_pairs = [(c, c ^ 1) for c in range(num_cols)]

    def bias_pairs(m):
        pairs = []
        for r in range(num_rows):
            for c in range(num_cols):
                e = c ^ m
                pairs.append((r * num_cols + c, (e >> 1) * num_cols + 2 * r + (e & 1)))
        return pairs

    def inner(z, res_mask, ln_gamma, ln_beta, w_q, w_k, w_v, w_b, w_g, w_o):
        row_len, cols, chan = z.shape
        heads = w_b.shape[1]
        sizes = (3 * cols, 7 * cols // 2, 4 * cols)
        col_idx = lax.axis_index('col')
        gamma, beta, wb_t = ln_gamma.reshape(1, chan), ln_beta.reshape(1, chan), w_b.T
        starts = [sum(CHUNKS[:i]) for i in range(len(CHUNKS))]
        head = normalize(z, gamma, beta, wb_t, 0, CHUNKS[:1], False)
        *tail, tail_bias, rest = normalize(z, gamma, beta, wb_t, CHUNKS[0], CHUNKS[1:], True)
        own = [head[0]] + tail
        halves = jnp.concatenate([head[1], tail_bias], axis=0).reshape(2, row_len // 2, heads, cols)
        info, w_kv, w_qg = make_plan(heads, sizes, res_mask.reshape(4, cols), gamma, beta, w_q, w_k, w_v, wb_t, w_g)
        weights = (w_kv, w_qg, w_o)

        parts = []
        for m in range(4):
            half = lax.dynamic_index_in_dim(halves, (col_idx ^ m) & 1, 0, keepdims=False)
            parts.append(lax.ppermute(half, ('row', 'col'), bias_pairs(m)))
        bias = lay_bias(info, parts)
        far, near = [], []
        for a in own:
            far.append(lax.ppermute(a, 'col', x_pairs))
        for a in (own[0], rest):
            near.append(lax.ppermute(a, 'col', core_pairs))
        out = None
        for i, (start, rows) in enumerate(zip(starts, CHUNKS)):
            diag = lax.ppermute(far[i], 'col', core_pairs)
            out = attend(heads, sizes, info, (own[i], near[min(i, 1)], far[i], diag), (0, start - CHUNKS[0] if i else 0, 0, 0), z, bias, weights, out, start, rows)
        return out

    return jax.shard_map(inner, mesh=mesh, in_specs=(tile_spec, P('dp'), P(), P(), P(), P(), P(), P(), P(), P()), out_specs=tile_spec, check_vma=False)
```

```python
import functools

import jax
import jax.numpy as jnp
from jax import lax
from jax.experimental import pallas as pl
from jax.experimental.pallas import tpu as pltpu
from jax.sharding import PartitionSpec as P


LN_EPS = 1e-5
CHUNKS = (16, 32, 48, 48, 48, 32, 32)
NORM_ROWS = 16
ATTEND_ROWS = 16
GROUP = 16
ATTEND_VMEM = (67043328, 40 * 1024 * 1024)
SCORE_BOUND = 1e8
VALUE_BOUND = 1e20
SUM_RANGE = (1e-10, 1e15)
NN = (((1,), (0,)), ((), ()))
NT = (((1,), (1,)), ((), ()))
f32, bf16 = jnp.float32, jnp.bfloat16
dot = functools.partial(lax.dot_general, preferred_element_type=f32)
VMEM_LIMIT = pltpu.CompilerParams(vmem_limit_bytes=67043328)


def whole(shape):
    return pl.BlockSpec(shape, lambda *_: (0,) * len(shape))


def plan_kernel(heads, sizes, mask_ref, gamma_ref, beta_ref, wq_ref, wk_ref, wv_ref, wb_ref, wg_ref, info_ref, wkv_ref, wqg_ref):
    chan = gamma_ref.shape[1]
    dim = chan // heads
    row_idx, col_idx = lax.axis_index('row'), lax.axis_index('col')
    wkv_ref[:, :chan], wkv_ref[:, chan:] = wk_ref[...], wv_ref[...]
    wqg_ref[:, :chan], wqg_ref[:, chan:] = wq_ref[...], wg_ref[...]
    reach = jnp.broadcast_to(jnp.abs(gamma_ref[...]) * chan ** 0.5 + jnp.abs(beta_ref[...]), (8, chan)) * 1.05
    q = jnp.dot(reach, jnp.abs(wq_ref[...].astype(f32)), preferred_element_type=f32) * dim ** -0.5
    k = jnp.dot(reach, jnp.abs(wk_ref[...].astype(f32)), preferred_element_type=f32)
    v = jnp.dot(reach, jnp.abs(wv_ref[...].astype(f32)), preferred_element_type=f32)
    b = reach[:1] * jnp.sum(jnp.abs(wb_ref[...].astype(f32)), axis=0, keepdims=True)
    s_bound = (jnp.sum(q * k) + jnp.sum(b)) * 1.1
    v_bound = jnp.max(v) * 1.1
    length = jnp.sum(mask_ref[...].astype(f32)).astype(jnp.int32)
    used = jnp.where(length <= sizes[0], sizes[0], sizes[1])
    info_ref[0] = col_idx
    info_ref[1] = 2 * row_idx + (col_idx & 1)
    info_ref[2] = length
    info_ref[3] = jnp.where((s_bound < SCORE_BOUND) & (v_bound < VALUE_BOUND), used, sizes[2])


def make_plan(heads, sizes, *args):
    chan = args[1].shape[1]
    return pl.pallas_call(
        functools.partial(plan_kernel, heads, sizes),
        in_specs=[whole(x.shape) for x in args],
        out_specs=[pl.BlockSpec(memory_space=pltpu.SMEM), whole((chan, 2 * chan)), whole((chan, 2 * chan))],
        out_shape=[jax.ShapeDtypeStruct((4,), jnp.int32)] + [jax.ShapeDtypeStruct((chan, 2 * chan), bf16)] * 2,
        compiler_params=VMEM_LIMIT,
        name="plan",
    )(*args)


def norm_kernel(places, z_ref, gamma_ref, beta_ref, wb_ref, *out_refs):
    rows, cols, chan = z_ref.shape
    b_ref = out_refs[len(places)]
    z = z_ref[...].reshape(rows * cols, chan)
    ones = jnp.full((chan, chan), 1.0 / chan, bf16)
    centered = z.astype(f32) - dot(z, ones, NN)
    var = jnp.mean(centered * centered, axis=-1, keepdims=True)
    a = (centered * lax.rsqrt(var + LN_EPS) * gamma_ref[...] + beta_ref[...]).astype(bf16)
    blocks = a.reshape(rows, cols, chan)
    i = pl.program_id(0)
    for out_ref, (lo, steps, offset) in zip(out_refs, places):
        @pl.when((i >= lo) & (i < lo + steps))
        def _():
            out_ref[...] = blocks[offset:offset + out_ref.shape[0]]
    for out_ref in out_refs[len(places) + 1:]:
        out_ref[...] = blocks
    b = dot(wb_ref[...], a, NT)
    for r in range(rows):
        b_ref[r] = b[:, r * cols:(r + 1) * cols].astype(bf16)


def normalize(z, gamma, beta, wb_t, start, chunks, joined):
    cols, chan = z.shape[1:]
    heads = wb_t.shape[0]
    step = NORM_ROWS
    first = start // step
    rows = sum(chunks)
    places, specs = [], []
    for i, c in enumerate(chunks):
        lo, offset = divmod(sum(chunks[:i]), step)
        steps = max(c // step, 1)
        places.append((lo, steps, offset))
        specs.append(pl.BlockSpec((min(step, c), cols, chan), lambda i, lo=lo, steps=steps: (jnp.clip(i - lo, 0, steps - 1), 0, 0)))
    specs.append(pl.BlockSpec((step, heads, cols), lambda i: (i, 0, 0)))
    shapes = [jax.ShapeDtypeStruct((c, cols, chan), bf16) for c in chunks] + [jax.ShapeDtypeStruct((rows, heads, cols), bf16)]
    if joined:
        specs.append(pl.BlockSpec((step, cols, chan), lambda i: (i, 0, 0)))
        shapes.append(jax.ShapeDtypeStruct((rows, cols, chan), bf16))
    return pl.pallas_call(
        functools.partial(norm_kernel, places),
        grid=(rows // step,),
        in_specs=[
            pl.BlockSpec((step, cols, chan), lambda i: (first + i, 0, 0)),
            whole((1, chan)), whole((1, chan)), whole(wb_t.shape),
        ],
        out_specs=specs,
        out_shape=shapes,
        compiler_params=VMEM_LIMIT,
        cost_estimate=pl.CostEstimate(flops=rows * cols * chan * 300, bytes_accessed=rows * cols * chan * 4, transcendentals=0),
        name="norm",
    )(z, gamma, beta, wb_t)


def bias_kernel(info_ref, *refs):
    parts, out_ref = refs[:-1], refs[-1]
    queries, heads, cols = parts[0].shape
    base, length = info_ref[1], info_ref[2]
    for m, part in enumerate(parts):
        first = pl.multiple_of((base ^ m) * cols, cols)
        key = first + lax.broadcasted_iota(jnp.int32, (cols, queries), 0)
        key_bias = jnp.where(key < length, 0.0, -1e9).astype(f32)
        b = part[...].astype(f32)
        for h in range(heads):
            out_ref[pl.ds(first, cols), h * queries:(h + 1) * queries] = b[:, h, :].T + key_bias


def lay_bias(info, parts):
    queries, heads, cols = parts[0].shape
    shape = (len(parts) * cols, heads * queries)
    return pl.pallas_call(
        bias_kernel,
        grid_spec=pltpu.PrefetchScalarGridSpec(
            num_scalar_prefetch=1, grid=(1,),
            in_specs=[whole(p.shape) for p in parts], out_specs=whole(shape),
        ),
        out_shape=jax.ShapeDtypeStruct(shape, f32),
        compiler_params=VMEM_LIMIT,
        name="bias",
    )(info, *parts)


def attend_kernel(heads, sizes, info_ref, *refs):
    blocks = refs[:4]
    z_ref, bias_ref, wkv_ref, wqg_ref, wo_ref = refs[4:9]
    out_ref, k_s, vt_s, q_s, g_s, p_s, l_s, o_s = refs[-8:]
    step, cols, chan = z_ref.shape
    dim = chan // heads
    col, used = info_ref[0], info_ref[3]

    @pl.when(pl.program_id(0) == 0)
    def _():
        q_s[...] = jnp.zeros_like(q_s)

    def project(i, carry):
        rows = pl.ds(GROUP * i, GROUP)
        for p, ref in enumerate(blocks):
            first = pl.multiple_of((col ^ p) * cols, cols)
            kv = dot(ref[rows].reshape(GROUP * cols, chan), wkv_ref[...], NN).astype(bf16)
            k_s[rows, pl.ds(first, cols), :] = kv[:, :chan].reshape(GROUP, cols, chan)
            v = kv[:, chan:].reshape(GROUP, cols, chan)
            for r in range(GROUP):
                vt_s[GROUP * i + r, :, pl.ds(first, cols)] = v[r].T
        qg = dot(blocks[0][rows].reshape(GROUP * cols, chan), wqg_ref[...], NN)
        q = (qg[:, :chan] * dim ** -0.5).astype(bf16).reshape(GROUP, cols, chan)
        for r in range(GROUP):
            q_t = q[r].T
            for h in range(heads):
                q_s[GROUP * i + r, h * dim:(h + 1) * dim, h * cols:(h + 1) * cols] = q_t[h * dim:(h + 1) * dim]
        g_s[rows] = jax.nn.sigmoid(qg[:, chan:]).reshape(GROUP, cols, chan)
        return carry

    lax.fori_loop(0, step // GROUP, project, 0)

    def run(keys, shift):
        def weigh(r, slot):
            s = dot(k_s[r, :keys, :], q_s[r], NN) + bias_ref[:keys, :]
            e = jnp.exp(s - jnp.max(s, axis=0, keepdims=True) if shift else s)
            l_s[r] = jnp.sum(e, axis=0, keepdims=True)
            p_s[slot, :keys, :] = e.astype(bf16)

        def mix(r, slot):
            o = dot(vt_s[r, :, :keys], p_s[slot, :keys, :], NN)
            inv = 1.0 / l_s[r]
            for h in range(heads):
                part = o[h * dim:(h + 1) * dim, h * cols:(h + 1) * cols]
                o_s[r, h * dim:(h + 1) * dim, :] = part * inv[:, h * cols:(h + 1) * cols]

        def pair(i, carry):
            r = 2 * i
            weigh(r, 0)
            mix(lax.rem(r + step - 1, step), 1)
            weigh(r + 1, 1)
            mix(r, 0)
            return carry

        def single(r, carry):
            weigh(r, 0)
            mix(r, 0)
            return carry

        if shift:
            lax.fori_loop(0, step, single, 0)
        else:
            lax.fori_loop(0, step // 2, pair, 0)
            mix(step - 1, 1)

    for keys in sizes[:-1]:
        pl.when(used == keys)(functools.partial(run, keys, False))
    l = l_s[...]
    fine = (used < sizes[-1]) & (jnp.min(l) > SUM_RANGE[0]) & (jnp.max(l) < SUM_RANGE[1])
    pl.when(jnp.logical_not(fine))(functools.partial(run, sizes[-1], True))

    def finish(i, carry):
        rows = pl.ds(GROUP * i, GROUP)
        gated = jnp.concatenate([(o_s[GROUP * i + r].T * g_s[GROUP * i + r]).astype(bf16) for r in range(GROUP)], axis=0)
        update = dot(gated, wo_ref[...], NN).reshape(GROUP, cols, chan)
        out_ref[rows] = (z_ref[rows].astype(f32) + update).astype(bf16)
        return carry

    lax.fori_loop(0, step // GROUP, finish, 0)


def attend(heads, sizes, info, blocks, skips, z, bias, weights, prev, start, rows):
    cols, chan = z.shape[1:]
    step = ATTEND_ROWS
    first = start // step
    keys = 4 * cols
    here = [pl.BlockSpec((step, cols, chan), lambda i, _, skip=skip: (skip // step + i, 0, 0)) for skip in skips]
    there = pl.BlockSpec((step, cols, chan), lambda i, _: (first + i, 0, 0))
    args = [info] + list(blocks) + [z, bias] + list(weights)
    specs = here + [there, whole(bias.shape)] + [whole(w.shape) for w in weights]
    alias = {}
    if prev is not None:
        alias = {len(args): 0}
        args.append(prev)
        specs.append(pl.BlockSpec(memory_space=pl.ANY))
    return pl.pallas_call(
        functools.partial(attend_kernel, heads, sizes),
        grid_spec=pltpu.PrefetchScalarGridSpec(
            num_scalar_prefetch=1, grid=(rows // step,), in_specs=specs, out_specs=there,
            scratch_shapes=[
                pltpu.VMEM((step, keys, chan), bf16),
                pltpu.VMEM((step, chan, keys), bf16),
                pltpu.VMEM((step, chan, heads * cols), bf16),
                pltpu.VMEM((step, cols, chan), f32),
                pltpu.VMEM((2, keys, heads * cols), bf16),
                pltpu.VMEM((step, 1, heads * cols), f32),
                pltpu.VMEM((step, chan, cols), f32),
            ],
        ),
        out_shape=jax.ShapeDtypeStruct(z.shape, z.dtype),
        input_output_aliases=alias,
        compiler_params=pltpu.CompilerParams(vmem_limit_bytes=ATTEND_VMEM[prev is not None]),
        cost_estimate=pl.CostEstimate(flops=rows * cols * chan * 8000, bytes_accessed=rows * cols * chan * 12, transcendentals=0),
        name="attend",
    )(*args)


def solution(mesh):
    tile_spec = P(('dp', 'row'), 'col', None)
    num_rows, num_cols = mesh.shape['row'], mesh.shape['col']
    x_pairs = [(c, c ^ 2) for c in range(num_cols)]
    core_pairs = [(c, c ^ 1) for c in range(num_cols)]

    def bias_pairs(m):
        pairs = []
        for r in range(num_rows):
            for c in range(num_cols):
                e = c ^ m
                pairs.append((r * num_cols + c, (e >> 1) * num_cols + 2 * r + (e & 1)))
        return pairs

    def inner(z, res_mask, ln_gamma, ln_beta, w_q, w_k, w_v, w_b, w_g, w_o):
        row_len, cols, chan = z.shape
        heads = w_b.shape[1]
        sizes = (3 * cols, 7 * cols // 2, 4 * cols)
        col_idx = lax.axis_index('col')
        gamma, beta, wb_t = ln_gamma.reshape(1, chan), ln_beta.reshape(1, chan), w_b.T
        starts = [sum(CHUNKS[:i]) for i in range(len(CHUNKS))]
        first, first_bias = normalize(z, gamma, beta, wb_t, 0, CHUNKS[:1], False)
        second, second_bias = normalize(z, gamma, beta, wb_t, starts[1], CHUNKS[1:2], False)
        *others, other_bias, rest = normalize(z, gamma, beta, wb_t, starts[2], CHUNKS[2:], True)
        own = [first, second] + others
        halves = jnp.concatenate([first_bias, second_bias, other_bias], axis=0).reshape(2, row_len // 2, heads, cols)
        info, w_kv, w_qg = make_plan(heads, sizes, res_mask.reshape(4, cols), gamma, beta, w_q, w_k, w_v, wb_t, w_g)
        weights = (w_kv, w_qg, w_o)

        parts = []
        for m in range(4):
            half = lax.dynamic_index_in_dim(halves, (col_idx ^ m) & 1, 0, keepdims=False)
            parts.append(lax.ppermute(half, ('row', 'col'), bias_pairs(m)))
        bias = lay_bias(info, parts)
        far, near = [], []
        for a in own:
            far.append(lax.ppermute(a, 'col', x_pairs))
        for a in (first, second, rest):
            near.append(lax.ppermute(a, 'col', core_pairs))
        out = None
        for i, (start, rows) in enumerate(zip(starts, CHUNKS)):
            diag = lax.ppermute(far[i], 'col', core_pairs)
            out = attend(heads, sizes, info, (own[i], near[min(i, 2)], far[i], diag), (0, max(start - starts[2], 0) if i > 1 else 0, 0, 0), z, bias, weights, out, start, rows)
        return out

    return jax.shard_map(inner, mesh=mesh, in_specs=(tile_spec, P('dp'), P(), P(), P(), P(), P(), P(), P(), P()), out_specs=tile_spec, check_vma=False)
```

```python
import functools

import jax
import jax.numpy as jnp
from jax import lax
from jax.experimental import pallas as pl
from jax.experimental.pallas import tpu as pltpu
from jax.sharding import PartitionSpec as P


LN_EPS = 1e-5
CHUNKS = (16, 32, 48, 48, 48, 32, 32)
NORM_ROWS = 16
ATTEND_ROWS = 16
GROUP = 16
ATTEND_VMEM = 67043328
SCORE_BOUND = 1e8
VALUE_BOUND = 1e20
SUM_RANGE = (1e-10, 1e15)
NN = (((1,), (0,)), ((), ()))
NT = (((1,), (1,)), ((), ()))
f32, bf16 = jnp.float32, jnp.bfloat16
dot = functools.partial(lax.dot_general, preferred_element_type=f32)
VMEM_LIMIT = pltpu.CompilerParams(vmem_limit_bytes=67043328)


def whole(shape):
    return pl.BlockSpec(shape, lambda *_: (0,) * len(shape))


def plan_kernel(heads, sizes, mask_ref, gamma_ref, beta_ref, wq_ref, wk_ref, wv_ref, wb_ref, wg_ref, info_ref, wkv_ref, wqg_ref):
    chan = gamma_ref.shape[1]
    dim = chan // heads
    col_idx = lax.axis_index('col')
    wkv_ref[:, :chan], wkv_ref[:, chan:] = wk_ref[...], wv_ref[...]
    wqg_ref[:, :chan], wqg_ref[:, chan:] = wq_ref[...], wg_ref[...]
    reach = jnp.broadcast_to(jnp.abs(gamma_ref[...]) * chan ** 0.5 + jnp.abs(beta_ref[...]), (8, chan)) * 1.05
    q = jnp.dot(reach, jnp.abs(wq_ref[...].astype(f32)), preferred_element_type=f32) * dim ** -0.5
    k = jnp.dot(reach, jnp.abs(wk_ref[...].astype(f32)), preferred_element_type=f32)
    v = jnp.dot(reach, jnp.abs(wv_ref[...].astype(f32)), preferred_element_type=f32)
    b = reach[:1] * jnp.sum(jnp.abs(wb_ref[...].astype(f32)), axis=0, keepdims=True)
    s_bound = (jnp.sum(q * k) + jnp.sum(b)) * 1.1
    v_bound = jnp.max(v) * 1.1
    length = jnp.sum(mask_ref[...].astype(f32)).astype(jnp.int32)
    used = jnp.where(length <= sizes[0], sizes[0], sizes[1])
    info_ref[0] = col_idx
    info_ref[1] = length
    info_ref[2] = jnp.where((s_bound < SCORE_BOUND) & (v_bound < VALUE_BOUND), used, sizes[2])


def make_plan(heads, sizes, *args):
    chan = args[1].shape[1]
    return pl.pallas_call(
        functools.partial(plan_kernel, heads, sizes),
        in_specs=[whole(x.shape) for x in args],
        out_specs=[pl.BlockSpec(memory_space=pltpu.SMEM), whole((chan, 2 * chan)), whole((chan, 2 * chan))],
        out_shape=[jax.ShapeDtypeStruct((3,), jnp.int32)] + [jax.ShapeDtypeStruct((chan, 2 * chan), bf16)] * 2,
        compiler_params=VMEM_LIMIT,
        name="plan",
    )(*args)


def norm_kernel(places, z_ref, gamma_ref, beta_ref, wb_ref, *out_refs):
    rows, cols, chan = z_ref.shape
    b_ref = out_refs[len(places)]
    z = z_ref[...].reshape(rows * cols, chan)
    ones = jnp.full((chan, chan), 1.0 / chan, bf16)
    centered = z.astype(f32) - dot(z, ones, NN)
    var = jnp.mean(centered * centered, axis=-1, keepdims=True)
    a = (centered * lax.rsqrt(var + LN_EPS) * gamma_ref[...] + beta_ref[...]).astype(bf16)
    blocks = a.reshape(rows, cols, chan)
    i = pl.program_id(0)
    for out_ref, (lo, steps, offset) in zip(out_refs, places):
        @pl.when((i >= lo) & (i < lo + steps))
        def _():
            out_ref[...] = blocks[offset:offset + out_ref.shape[0]]
    for out_ref in out_refs[len(places) + 1:]:
        out_ref[...] = blocks
    b = dot(wb_ref[...], a, NT)
    for r in range(rows):
        b_ref[r] = b[:, r * cols:(r + 1) * cols].astype(bf16)


def normalize(z, gamma, beta, wb_t, start, chunks, joined):
    cols, chan = z.shape[1:]
    heads = wb_t.shape[0]
    step = NORM_ROWS
    first = start // step
    rows = sum(chunks)
    places, specs = [], []
    for i, c in enumerate(chunks):
        lo, offset = divmod(sum(chunks[:i]), step)
        steps = max(c // step, 1)
        places.append((lo, steps, offset))
        specs.append(pl.BlockSpec((min(step, c), cols, chan), lambda i, lo=lo, steps=steps: (jnp.clip(i - lo, 0, steps - 1), 0, 0)))
    specs.append(pl.BlockSpec((step, heads, cols), lambda i: (i, 0, 0)))
    shapes = [jax.ShapeDtypeStruct((c, cols, chan), bf16) for c in chunks] + [jax.ShapeDtypeStruct((rows, heads, cols), bf16)]
    if joined:
        specs.append(pl.BlockSpec((step, cols, chan), lambda i: (i, 0, 0)))
        shapes.append(jax.ShapeDtypeStruct((rows, cols, chan), bf16))
    return pl.pallas_call(
        functools.partial(norm_kernel, places),
        grid=(rows // step,),
        in_specs=[
            pl.BlockSpec((step, cols, chan), lambda i: (first + i, 0, 0)),
            whole((1, chan)), whole((1, chan)), whole(wb_t.shape),
        ],
        out_specs=specs,
        out_shape=shapes,
        compiler_params=VMEM_LIMIT,
        cost_estimate=pl.CostEstimate(flops=rows * cols * chan * 300, bytes_accessed=rows * cols * chan * 4, transcendentals=0),
        name="norm",
    )(z, gamma, beta, wb_t)


def bias_kernel(info_ref, *refs):
    parts, out_ref = refs[:-1], refs[-1]
    queries, heads, cols = parts[0].shape
    col, length = info_ref[0], info_ref[1]
    for m, part in enumerate(parts):
        first = pl.multiple_of((col ^ m) * cols, cols)
        key = first + lax.broadcasted_iota(jnp.int32, (cols, queries), 0)
        key_bias = jnp.where(key < length, 0.0, -1e9).astype(f32)
        b = part[...].astype(f32)
        for h in range(heads):
            out_ref[pl.ds(first, cols), h * queries:(h + 1) * queries] = b[:, h, :].T + key_bias


def lay_bias(info, parts):
    queries, heads, cols = parts[0].shape
    shape = (len(parts) * cols, heads * queries)
    return pl.pallas_call(
        bias_kernel,
        grid_spec=pltpu.PrefetchScalarGridSpec(
            num_scalar_prefetch=1, grid=(1,),
            in_specs=[whole(p.shape) for p in parts], out_specs=whole(shape),
        ),
        out_shape=jax.ShapeDtypeStruct(shape, f32),
        compiler_params=VMEM_LIMIT,
        name="bias",
    )(info, *parts)


def attend_kernel(heads, sizes, info_ref, *refs):
    blocks = refs[:4]
    z_ref, bias_ref, wkv_ref, wqg_ref, wo_ref = refs[4:9]
    out_ref, k_s, vt_s, q_s, g_s, p_s, l_s, o_s = refs[-8:]
    step, cols, chan = z_ref.shape
    dim = chan // heads
    col, used = info_ref[0], info_ref[2]

    @pl.when(pl.program_id(0) == 0)
    def _():
        q_s[...] = jnp.zeros_like(q_s)

    def project(i, carry):
        rows = pl.ds(GROUP * i, GROUP)
        for p, ref in enumerate(blocks):
            first = pl.multiple_of((col ^ p) * cols, cols)
            kv = dot(ref[rows].reshape(GROUP * cols, chan), wkv_ref[...], NN).astype(bf16)
            k_s[rows, pl.ds(first, cols), :] = kv[:, :chan].reshape(GROUP, cols, chan)
            v = kv[:, chan:].reshape(GROUP, cols, chan)
            for r in range(GROUP):
                vt_s[GROUP * i + r, :, pl.ds(first, cols)] = v[r].T
        qg = dot(blocks[0][rows].reshape(GROUP * cols, chan), wqg_ref[...], NN)
        q = (qg[:, :chan] * dim ** -0.5).astype(bf16).reshape(GROUP, cols, chan)
        for r in range(GROUP):
            q_t = q[r].T
            for h in range(heads):
                q_s[GROUP * i + r, h * dim:(h + 1) * dim, h * cols:(h + 1) * cols] = q_t[h * dim:(h + 1) * dim]
        g_s[rows] = jax.nn.sigmoid(qg[:, chan:]).reshape(GROUP, cols, chan)
        return carry

    lax.fori_loop(0, step // GROUP, project, 0)

    def run(keys, shift):
        def weigh(r, slot):
            s = dot(k_s[r, :keys, :], q_s[r], NN) + bias_ref[:keys, :]
            e = jnp.exp(s - jnp.max(s, axis=0, keepdims=True) if shift else s)
            l_s[r] = jnp.sum(e, axis=0, keepdims=True)
            p_s[slot, :keys, :] = e.astype(bf16)

        def mix(r, slot):
            o = dot(vt_s[r, :, :keys], p_s[slot, :keys, :], NN)
            inv = 1.0 / l_s[r]
            for h in range(heads):
                part = o[h * dim:(h + 1) * dim, h * cols:(h + 1) * cols]
                o_s[r, h * dim:(h + 1) * dim, :] = part * inv[:, h * cols:(h + 1) * cols]

        def pair(i, carry):
            r = 2 * i
            weigh(r, 0)
            mix(lax.rem(r + step - 1, step), 1)
            weigh(r + 1, 1)
            mix(r, 0)
            return carry

        def single(r, carry):
            weigh(r, 0)
            mix(r, 0)
            return carry

        if shift:
            lax.fori_loop(0, step, single, 0)
        else:
            lax.fori_loop(0, step // 2, pair, 0)
            mix(step - 1, 1)

    for keys in sizes[:-1]:
        pl.when(used == keys)(functools.partial(run, keys, False))
    l = l_s[...]
    fine = (used < sizes[-1]) & (jnp.min(l) > SUM_RANGE[0]) & (jnp.max(l) < SUM_RANGE[1])
    pl.when(jnp.logical_not(fine))(functools.partial(run, sizes[-1], True))

    def finish(i, carry):
        rows = pl.ds(GROUP * i, GROUP)
        gated = jnp.concatenate([(o_s[GROUP * i + r].T * g_s[GROUP * i + r]).astype(bf16) for r in range(GROUP)], axis=0)
        update = dot(gated, wo_ref[...], NN).reshape(GROUP, cols, chan)
        out_ref[rows] = (z_ref[rows].astype(f32) + update).astype(bf16)
        return carry

    lax.fori_loop(0, step // GROUP, finish, 0)


def attend(heads, sizes, info, blocks, skips, z, bias, weights, prev, start, rows):
    cols, chan = z.shape[1:]
    step = ATTEND_ROWS
    first = start // step
    keys = 4 * cols
    here = [pl.BlockSpec((step, cols, chan), lambda i, _, skip=skip: (skip // step + i, 0, 0)) for skip in skips]
    there = pl.BlockSpec((step, cols, chan), lambda i, _: (first + i, 0, 0))
    args = [info] + list(blocks) + [z, bias] + list(weights)
    specs = here + [there, whole(bias.shape)] + [whole(w.shape) for w in weights]
    alias = {}
    if prev is not None:
        alias = {len(args): 0}
        args.append(prev)
        specs.append(pl.BlockSpec(memory_space=pl.ANY))
    return pl.pallas_call(
        functools.partial(attend_kernel, heads, sizes),
        grid_spec=pltpu.PrefetchScalarGridSpec(
            num_scalar_prefetch=1, grid=(rows // step,), in_specs=specs, out_specs=there,
            scratch_shapes=[
                pltpu.VMEM((step, keys, chan), bf16),
                pltpu.VMEM((step, chan, keys), bf16),
                pltpu.VMEM((step, chan, heads * cols), bf16),
                pltpu.VMEM((step, cols, chan), f32),
                pltpu.VMEM((2, keys, heads * cols), bf16),
                pltpu.VMEM((step, 1, heads * cols), f32),
                pltpu.VMEM((step, chan, cols), f32),
            ],
        ),
        out_shape=jax.ShapeDtypeStruct(z.shape, z.dtype),
        input_output_aliases=alias,
        compiler_params=pltpu.CompilerParams(vmem_limit_bytes=ATTEND_VMEM),
        cost_estimate=pl.CostEstimate(flops=rows * cols * chan * 8000, bytes_accessed=rows * cols * chan * 12, transcendentals=0),
        name="attend",
    )(*args)


def solution(mesh):
    tile_spec = P(('dp', 'row'), 'col', None)
    num_cols = mesh.shape['col']
    x_pairs = [(c, c ^ 2) for c in range(num_cols)]
    core_pairs = [(c, c ^ 1) for c in range(num_cols)]

    def inner(z, res_mask, ln_gamma, ln_beta, w_q, w_k, w_v, w_b, w_g, w_o):
        _, cols, chan = z.shape
        heads = w_b.shape[1]
        sizes = (3 * cols, 7 * cols // 2, 4 * cols)
        col_idx = lax.axis_index('col')
        gamma, beta, wb_t = ln_gamma.reshape(1, chan), ln_beta.reshape(1, chan), w_b.T
        starts = [sum(CHUNKS[:i]) for i in range(len(CHUNKS))]
        first, first_bias = normalize(z, gamma, beta, wb_t, 0, CHUNKS[:1], False)
        second, second_bias = normalize(z, gamma, beta, wb_t, starts[1], CHUNKS[1:2], False)
        *others, other_bias, rest = normalize(z, gamma, beta, wb_t, starts[2], CHUNKS[2:], True)
        own = [first, second] + others
        bias_tile = jnp.concatenate([first_bias, second_bias, other_bias], axis=0)
        other_tile = lax.ppermute(bias_tile, 'row', [(0, 1), (1, 0)])
        info, w_kv, w_qg = make_plan(heads, sizes, res_mask.reshape(4, cols), gamma, beta, w_q, w_k, w_v, wb_t, w_g)
        weights = (w_kv, w_qg, w_o)

        halves = [bias_tile[:cols], bias_tile[cols:], other_tile[:cols], other_tile[cols:]]
        parts = []
        for m in range(num_cols):
            place = (col_idx ^ m) ^ (2 * lax.axis_index('row'))
            send = jnp.where(place & 2, jnp.where(place & 1, halves[3], halves[2]), jnp.where(place & 1, halves[1], halves[0]))
            parts.append(lax.ppermute(send, 'col', [(c, c ^ m) for c in range(num_cols)]) if m else send)
        bias = lay_bias(info, parts)
        far, near = [], []
        for a in own:
            far.append(lax.ppermute(a, 'col', x_pairs))
        for a in (first, second, rest):
            near.append(lax.ppermute(a, 'col', core_pairs))
        out = None
        for i, (start, rows) in enumerate(zip(starts, CHUNKS)):
            diag = lax.ppermute(far[i], 'col', core_pairs)
            out = attend(heads, sizes, info, (own[i], near[min(i, 2)], far[i], diag), (0, max(start - starts[2], 0) if i > 1 else 0, 0, 0), z, bias, weights, out, start, rows)
        return out

    return jax.shard_map(inner, mesh=mesh, in_specs=(tile_spec, P('dp'), P(), P(), P(), P(), P(), P(), P(), P()), out_specs=tile_spec, check_vma=False)
```

```python
import functools

import jax
import jax.numpy as jnp
from jax import lax
from jax.experimental import pallas as pl
from jax.experimental.pallas import tpu as pltpu
from jax.sharding import PartitionSpec as P


LN_EPS = 1e-5
CHUNKS = (16, 32, 48, 48, 48, 32, 32)
NORM_ROWS = 16
ATTEND_ROWS = 16
GROUP = 16
SCORE_BOUND = 1e8
VALUE_BOUND = 1e20
SUM_RANGE = (1e-10, 1e15)
NN = (((1,), (0,)), ((), ()))
NT = (((1,), (1,)), ((), ()))
f32, bf16 = jnp.float32, jnp.bfloat16
dot = functools.partial(lax.dot_general, preferred_element_type=f32)
VMEM_LIMIT = pltpu.CompilerParams(vmem_limit_bytes=57 * 1024 * 1024)


def whole(shape):
    return pl.BlockSpec(shape, lambda *_: (0,) * len(shape))


def plan_kernel(heads, sizes, mask_ref, gamma_ref, beta_ref, wq_ref, wk_ref, wv_ref, wb_ref, wg_ref, info_ref, wkv_ref, wqg_ref):
    chan = gamma_ref.shape[1]
    dim = chan // heads
    col_idx = lax.axis_index('col')
    wkv_ref[:, :chan], wkv_ref[:, chan:] = wk_ref[...], wv_ref[...]
    wqg_ref[:, :chan], wqg_ref[:, chan:] = wq_ref[...], wg_ref[...]
    reach = jnp.broadcast_to(jnp.abs(gamma_ref[...]) * chan ** 0.5 + jnp.abs(beta_ref[...]), (8, chan)) * 1.05
    q = jnp.dot(reach, jnp.abs(wq_ref[...].astype(f32)), preferred_element_type=f32) * dim ** -0.5
    k = jnp.dot(reach, jnp.abs(wk_ref[...].astype(f32)), preferred_element_type=f32)
    v = jnp.dot(reach, jnp.abs(wv_ref[...].astype(f32)), preferred_element_type=f32)
    b = reach[:1] * jnp.sum(jnp.abs(wb_ref[...].astype(f32)), axis=0, keepdims=True)
    s_bound = (jnp.sum(q * k) + jnp.sum(b)) * 1.1
    v_bound = jnp.max(v) * 1.1
    length = jnp.sum(mask_ref[...].astype(f32)).astype(jnp.int32)
    used = jnp.where(length <= sizes[0], sizes[0], sizes[1])
    info_ref[0] = col_idx
    info_ref[1] = length
    info_ref[2] = jnp.where((s_bound < SCORE_BOUND) & (v_bound < VALUE_BOUND), used, sizes[2])


def make_plan(heads, sizes, *args):
    chan = args[1].shape[1]
    return pl.pallas_call(
        functools.partial(plan_kernel, heads, sizes),
        in_specs=[whole(x.shape) for x in args],
        out_specs=[pl.BlockSpec(memory_space=pltpu.SMEM), whole((chan, 2 * chan)), whole((chan, 2 * chan))],
        out_shape=[jax.ShapeDtypeStruct((3,), jnp.int32)] + [jax.ShapeDtypeStruct((chan, 2 * chan), bf16)] * 2,
        compiler_params=VMEM_LIMIT,
        name="plan",
    )(*args)


def norm_kernel(places, aliased, z_ref, gamma_ref, beta_ref, wb_ref, *out_refs):
    out_refs = out_refs[1:] if aliased else out_refs
    rows, cols, chan = z_ref.shape
    b_ref = out_refs[len(places)]
    z = z_ref[...].reshape(rows * cols, chan)
    ones = jnp.full((chan, chan), 1.0 / chan, bf16)
    centered = z.astype(f32) - dot(z, ones, NN)
    var = jnp.mean(centered * centered, axis=-1, keepdims=True)
    a = (centered * lax.rsqrt(var + LN_EPS) * gamma_ref[...] + beta_ref[...]).astype(bf16)
    blocks = a.reshape(rows, cols, chan)
    i = pl.program_id(0)
    for out_ref, (lo, steps, offset) in zip(out_refs, places):
        @pl.when((i >= lo) & (i < lo + steps))
        def _():
            out_ref[...] = blocks[offset:offset + out_ref.shape[0]]
    for out_ref in out_refs[len(places) + 1:]:
        out_ref[...] = blocks
    b = dot(wb_ref[...], a, NT)
    for r in range(rows):
        b_ref[r] = b[:, r * cols:(r + 1) * cols].astype(bf16)


def normalize(z, gamma, beta, wb_t, prev, start, chunks, joined):
    total, cols, chan = z.shape
    heads = wb_t.shape[0]
    step = NORM_ROWS
    first = start // step
    rows = sum(chunks)
    places, specs = [], []
    for i, c in enumerate(chunks):
        lo, offset = divmod(sum(chunks[:i]), step)
        steps = max(c // step, 1)
        places.append((lo, steps, offset))
        specs.append(pl.BlockSpec((min(step, c), cols, chan), lambda i, lo=lo, steps=steps: (jnp.clip(i - lo, 0, steps - 1), 0, 0)))
    specs.append(pl.BlockSpec((step, heads, cols), lambda i: (first + i, 0, 0)))
    shapes = [jax.ShapeDtypeStruct((c, cols, chan), bf16) for c in chunks] + [jax.ShapeDtypeStruct((total, heads, cols), bf16)]
    if joined:
        specs.append(pl.BlockSpec((step, cols, chan), lambda i: (i, 0, 0)))
        shapes.append(jax.ShapeDtypeStruct((rows, cols, chan), bf16))
    args = [z, gamma, beta, wb_t]
    in_specs = [pl.BlockSpec((step, cols, chan), lambda i: (first + i, 0, 0))] + [whole(x.shape) for x in args[1:]]
    alias = {}
    if prev is not None:
        alias = {len(args): len(chunks)}
        args.append(prev)
        in_specs.append(pl.BlockSpec(memory_space=pl.ANY))
    return pl.pallas_call(
        functools.partial(norm_kernel, places, prev is not None),
        grid=(rows // step,),
        in_specs=in_specs,
        out_specs=specs,
        out_shape=shapes,
        input_output_aliases=alias,
        compiler_params=VMEM_LIMIT,
        cost_estimate=pl.CostEstimate(flops=rows * cols * chan * 300, bytes_accessed=rows * cols * chan * 4, transcendentals=0),
        name="norm",
    )(*args)


def bias_kernel(info_ref, *refs):
    parts, out_ref = refs[:-1], refs[-1]
    queries, heads, cols = parts[0].shape
    col, length = info_ref[0], info_ref[1]
    for m, part in enumerate(parts):
        first = pl.multiple_of((col ^ m) * cols, cols)
        key = first + lax.broadcasted_iota(jnp.int32, (cols, queries), 0)
        key_bias = jnp.where(key < length, 0.0, -1e9).astype(f32)
        b = part[...].astype(f32)
        for h in range(heads):
            out_ref[pl.ds(first, cols), h * queries:(h + 1) * queries] = b[:, h, :].T + key_bias


def lay_bias(info, parts):
    queries, heads, cols = parts[0].shape
    shape = (len(parts) * cols, heads * queries)
    return pl.pallas_call(
        bias_kernel,
        grid_spec=pltpu.PrefetchScalarGridSpec(
            num_scalar_prefetch=1, grid=(1,),
            in_specs=[whole(p.shape) for p in parts], out_specs=whole(shape),
        ),
        out_shape=jax.ShapeDtypeStruct(shape, f32),
        compiler_params=VMEM_LIMIT,
        name="bias",
    )(info, *parts)


def attend_kernel(heads, sizes, info_ref, *refs):
    blocks = refs[:4]
    z_ref, bias_ref, wkv_ref, wqg_ref, wo_ref = refs[4:9]
    out_ref, k_s, vt_s, q_s, g_s, p_s, l_s, o_s = refs[-8:]
    step, cols, chan = z_ref.shape
    dim = chan // heads
    col, used = info_ref[0], info_ref[2]

    @pl.when(pl.program_id(0) == 0)
    def _():
        q_s[...] = jnp.zeros_like(q_s)

    def project(i, carry):
        rows = pl.ds(GROUP * i, GROUP)
        for p, ref in enumerate(blocks):
            first = pl.multiple_of((col ^ p) * cols, cols)
            kv = dot(ref[rows].reshape(GROUP * cols, chan), wkv_ref[...], NN).astype(bf16)
            k_s[rows, pl.ds(first, cols), :] = kv[:, :chan].reshape(GROUP, cols, chan)
            v = kv[:, chan:].reshape(GROUP, cols, chan)
            for r in range(GROUP):
                vt_s[GROUP * i + r, :, pl.ds(first, cols)] = v[r].T
        qg = dot(blocks[0][rows].reshape(GROUP * cols, chan), wqg_ref[...], NN)
        q = (qg[:, :chan] * dim ** -0.5).astype(bf16).reshape(GROUP, cols, chan)
        for r in range(GROUP):
            q_t = q[r].T
            for h in range(heads):
                q_s[GROUP * i + r, h * dim:(h + 1) * dim, h * cols:(h + 1) * cols] = q_t[h * dim:(h + 1) * dim]
        g_s[rows] = jax.nn.sigmoid(qg[:, chan:]).reshape(GROUP, cols, chan)
        return carry

    lax.fori_loop(0, step // GROUP, project, 0)

    def run(keys, shift):
        def weigh(r, slot):
            s = dot(k_s[r, :keys, :], q_s[r], NN) + bias_ref[:keys, :]
            e = jnp.exp(s - jnp.max(s, axis=0, keepdims=True) if shift else s)
            l_s[r] = jnp.sum(e, axis=0, keepdims=True)
            p_s[slot, :keys, :] = e.astype(bf16)

        def mix(r, slot):
            o = dot(vt_s[r, :, :keys], p_s[slot, :keys, :], NN)
            inv = 1.0 / l_s[r]
            for h in range(heads):
                part = o[h * dim:(h + 1) * dim, h * cols:(h + 1) * cols]
                o_s[r, h * dim:(h + 1) * dim, :] = part * inv[:, h * cols:(h + 1) * cols]

        def pair(i, carry):
            r = 2 * i
            weigh(r, 0)
            mix(lax.rem(r + step - 1, step), 1)
            weigh(r + 1, 1)
            mix(r, 0)
            return carry

        def single(r, carry):
            weigh(r, 0)
            mix(r, 0)
            return carry

        if shift:
            lax.fori_loop(0, step, single, 0)
        else:
            lax.fori_loop(0, step // 2, pair, 0)
            mix(step - 1, 1)

    for keys in sizes[:-1]:
        pl.when(used == keys)(functools.partial(run, keys, False))
    l = l_s[...]
    fine = (used < sizes[-1]) & (jnp.min(l) > SUM_RANGE[0]) & (jnp.max(l) < SUM_RANGE[1])
    pl.when(jnp.logical_not(fine))(functools.partial(run, sizes[-1], True))

    def finish(i, carry):
        rows = pl.ds(GROUP * i, GROUP)
        gated = jnp.concatenate([(o_s[GROUP * i + r].T * g_s[GROUP * i + r]).astype(bf16) for r in range(GROUP)], axis=0)
        update = dot(gated, wo_ref[...], NN).reshape(GROUP, cols, chan)
        out_ref[rows] = (z_ref[rows].astype(f32) + update).astype(bf16)
        return carry

    lax.fori_loop(0, step // GROUP, finish, 0)


def attend(heads, sizes, info, blocks, skips, z, bias, weights, prev, start, rows):
    cols, chan = z.shape[1:]
    step = ATTEND_ROWS
    first = start // step
    keys = 4 * cols
    here = [pl.BlockSpec((step, cols, chan), lambda i, _, skip=skip: (skip // step + i, 0, 0)) for skip in skips]
    there = pl.BlockSpec((step, cols, chan), lambda i, _: (first + i, 0, 0))
    args = [info] + list(blocks) + [z, bias] + list(weights)
    specs = here + [there, whole(bias.shape)] + [whole(w.shape) for w in weights]
    alias = {}
    if prev is not None:
        alias = {len(args): 0}
        args.append(prev)
        specs.append(pl.BlockSpec(memory_space=pl.ANY))
    return pl.pallas_call(
        functools.partial(attend_kernel, heads, sizes),
        grid_spec=pltpu.PrefetchScalarGridSpec(
            num_scalar_prefetch=1, grid=(rows // step,), in_specs=specs, out_specs=there,
            scratch_shapes=[
                pltpu.VMEM((step, keys, chan), bf16),
                pltpu.VMEM((step, chan, keys), bf16),
                pltpu.VMEM((step, chan, heads * cols), bf16),
                pltpu.VMEM((step, cols, chan), f32),
                pltpu.VMEM((2, keys, heads * cols), bf16),
                pltpu.VMEM((step, 1, heads * cols), f32),
                pltpu.VMEM((step, chan, cols), f32),
            ],
        ),
        out_shape=jax.ShapeDtypeStruct(z.shape, z.dtype),
        input_output_aliases=alias,
        compiler_params=VMEM_LIMIT,
        cost_estimate=pl.CostEstimate(flops=rows * cols * chan * 8000, bytes_accessed=rows * cols * chan * 12, transcendentals=0),
        name="attend",
    )(*args)


def solution(mesh):
    tile_spec = P(('dp', 'row'), 'col', None)
    num_cols = mesh.shape['col']
    x_pairs = [(c, c ^ 2) for c in range(num_cols)]
    core_pairs = [(c, c ^ 1) for c in range(num_cols)]

    def inner(z, res_mask, ln_gamma, ln_beta, w_q, w_k, w_v, w_b, w_g, w_o):
        _, cols, chan = z.shape
        heads = w_b.shape[1]
        sizes = (3 * cols, 7 * cols // 2, 4 * cols)
        col_idx = lax.axis_index('col')
        gamma, beta, wb_t = ln_gamma.reshape(1, chan), ln_beta.reshape(1, chan), w_b.T
        starts = [sum(CHUNKS[:i]) for i in range(len(CHUNKS))]
        first, bias_tile = normalize(z, gamma, beta, wb_t, None, 0, CHUNKS[:1], False)
        second, bias_tile = normalize(z, gamma, beta, wb_t, bias_tile, starts[1], CHUNKS[1:2], False)
        *others, bias_tile, rest = normalize(z, gamma, beta, wb_t, bias_tile, starts[2], CHUNKS[2:], True)
        own = [first, second] + others
        other_tile = lax.ppermute(bias_tile, 'row', [(0, 1), (1, 0)])
        info, w_kv, w_qg = make_plan(heads, sizes, res_mask.reshape(4, cols), gamma, beta, w_q, w_k, w_v, wb_t, w_g)
        weights = (w_kv, w_qg, w_o)

        halves = [bias_tile[:cols], bias_tile[cols:], other_tile[:cols], other_tile[cols:]]
        parts = []
        for m in range(num_cols):
            place = (col_idx ^ m) ^ (2 * lax.axis_index('row'))
            send = jnp.where(place & 2, jnp.where(place & 1, halves[3], halves[2]), jnp.where(place & 1, halves[1], halves[0]))
            parts.append(lax.ppermute(send, 'col', [(c, c ^ m) for c in range(num_cols)]) if m else send)
        bias = lay_bias(info, parts)
        far, near = [], []
        for a in own:
            far.append(lax.ppermute(a, 'col', x_pairs))
        for a in (first, second, rest):
            near.append(lax.ppermute(a, 'col', core_pairs))
        out = None
        for i, (start, rows) in enumerate(zip(starts, CHUNKS)):
            diag = lax.ppermute(far[i], 'col', core_pairs)
            out = attend(heads, sizes, info, (own[i], near[min(i, 2)], far[i], diag), (0, max(start - starts[2], 0) if i > 1 else 0, 0, 0), z, bias, weights, out, start, rows)
        return out

    return jax.shard_map(inner, mesh=mesh, in_specs=(tile_spec, P('dp'), P(), P(), P(), P(), P(), P(), P(), P()), out_specs=tile_spec, check_vma=False)
```

```python
import functools

import jax
import jax.numpy as jnp
from jax import lax
from jax.experimental import pallas as pl
from jax.experimental.pallas import tpu as pltpu
from jax.sharding import PartitionSpec as P


LN_EPS = 1e-5
CHUNKS = (16, 32, 48, 48, 48, 32, 32)
NORM_ROWS = 16
ATTEND_ROWS = 16
GROUP = 16
ATTEND_VMEM = (67043328, 40 * 1024 * 1024)
SCORE_BOUND = 1e8
VALUE_BOUND = 1e20
SUM_RANGE = (1e-10, 1e15)
NN = (((1,), (0,)), ((), ()))
NT = (((1,), (1,)), ((), ()))
f32, bf16 = jnp.float32, jnp.bfloat16
dot = functools.partial(lax.dot_general, preferred_element_type=f32)
VMEM_LIMIT = pltpu.CompilerParams(vmem_limit_bytes=67043328)


def whole(shape):
    return pl.BlockSpec(shape, lambda *_: (0,) * len(shape))


def plan_kernel(heads, sizes, mask_ref, gamma_ref, beta_ref, wq_ref, wk_ref, wv_ref, wb_ref, wg_ref, info_ref, wkv_ref, wqg_ref):
    chan = gamma_ref.shape[1]
    dim = chan // heads
    col_idx = lax.axis_index('col')
    wkv_ref[:, :chan], wkv_ref[:, chan:] = wk_ref[...], wv_ref[...]
    wqg_ref[:, :chan], wqg_ref[:, chan:] = wq_ref[...], wg_ref[...]
    reach = jnp.broadcast_to(jnp.abs(gamma_ref[...]) * chan ** 0.5 + jnp.abs(beta_ref[...]), (8, chan)) * 1.05
    q = jnp.dot(reach, jnp.abs(wq_ref[...].astype(f32)), preferred_element_type=f32) * dim ** -0.5
    k = jnp.dot(reach, jnp.abs(wk_ref[...].astype(f32)), preferred_element_type=f32)
    v = jnp.dot(reach, jnp.abs(wv_ref[...].astype(f32)), preferred_element_type=f32)
    b = reach[:1] * jnp.sum(jnp.abs(wb_ref[...].astype(f32)), axis=0, keepdims=True)
    s_bound = (jnp.sum(q * k) + jnp.sum(b)) * 1.1
    v_bound = jnp.max(v) * 1.1
    length = jnp.sum(mask_ref[...].astype(f32)).astype(jnp.int32)
    used = jnp.where(length <= sizes[0], sizes[0], sizes[1])
    info_ref[0] = col_idx
    info_ref[1] = length
    info_ref[2] = jnp.where((s_bound < SCORE_BOUND) & (v_bound < VALUE_BOUND), used, sizes[2])


def make_plan(heads, sizes, *args):
    chan = args[1].shape[1]
    return pl.pallas_call(
        functools.partial(plan_kernel, heads, sizes),
        in_specs=[whole(x.shape) for x in args],
        out_specs=[pl.BlockSpec(memory_space=pltpu.SMEM), whole((chan, 2 * chan)), whole((chan, 2 * chan))],
        out_shape=[jax.ShapeDtypeStruct((3,), jnp.int32)] + [jax.ShapeDtypeStruct((chan, 2 * chan), bf16)] * 2,
        compiler_params=VMEM_LIMIT,
        name="plan",
    )(*args)


def norm_kernel(places, aliased, z_ref, gamma_ref, beta_ref, wb_ref, *out_refs):
    out_refs = out_refs[1:] if aliased else out_refs
    rows, cols, chan = z_ref.shape
    b_ref = out_refs[len(places)]
    z = z_ref[...].reshape(rows * cols, chan)
    ones = jnp.full((chan, chan), 1.0 / chan, bf16)
    centered = z.astype(f32) - dot(z, ones, NN)
    var = jnp.mean(centered * centered, axis=-1, keepdims=True)
    a = (centered * lax.rsqrt(var + LN_EPS) * gamma_ref[...] + beta_ref[...]).astype(bf16)
    blocks = a.reshape(rows, cols, chan)
    i = pl.program_id(0)
    for out_ref, (lo, steps, offset) in zip(out_refs, places):
        @pl.when((i >= lo) & (i < lo + steps))
        def _():
            out_ref[...] = blocks[offset:offset + out_ref.shape[0]]
    for out_ref in out_refs[len(places) + 1:]:
        out_ref[...] = blocks
    b = dot(wb_ref[...], a, NT)
    for r in range(rows):
        b_ref[r] = b[:, r * cols:(r + 1) * cols].astype(bf16)


def normalize(z, gamma, beta, wb_t, prev, start, chunks, joined):
    total, cols, chan = z.shape
    heads = wb_t.shape[0]
    step = NORM_ROWS
    first = start // step
    rows = sum(chunks)
    places, specs = [], []
    for i, c in enumerate(chunks):
        lo, offset = divmod(sum(chunks[:i]), step)
        steps = max(c // step, 1)
        places.append((lo, steps, offset))
        specs.append(pl.BlockSpec((min(step, c), cols, chan), lambda i, lo=lo, steps=steps: (jnp.clip(i - lo, 0, steps - 1), 0, 0)))
    specs.append(pl.BlockSpec((step, heads, cols), lambda i: (first + i, 0, 0)))
    shapes = [jax.ShapeDtypeStruct((c, cols, chan), bf16) for c in chunks] + [jax.ShapeDtypeStruct((total, heads, cols), bf16)]
    if joined:
        specs.append(pl.BlockSpec((step, cols, chan), lambda i: (i, 0, 0)))
        shapes.append(jax.ShapeDtypeStruct((rows, cols, chan), bf16))
    args = [z, gamma, beta, wb_t]
    in_specs = [pl.BlockSpec((step, cols, chan), lambda i: (first + i, 0, 0))] + [whole(x.shape) for x in args[1:]]
    alias = {}
    if prev is not None:
        alias = {len(args): len(chunks)}
        args.append(prev)
        in_specs.append(pl.BlockSpec(memory_space=pl.ANY))
    return pl.pallas_call(
        functools.partial(norm_kernel, places, prev is not None),
        grid=(rows // step,),
        in_specs=in_specs,
        out_specs=specs,
        out_shape=shapes,
        input_output_aliases=alias,
        compiler_params=VMEM_LIMIT,
        cost_estimate=pl.CostEstimate(flops=rows * cols * chan * 300, bytes_accessed=rows * cols * chan * 4, transcendentals=0),
        name="norm",
    )(*args)


def bias_kernel(info_ref, *refs):
    parts, out_ref = refs[:-1], refs[-1]
    queries, heads, cols = parts[0].shape
    col, length = info_ref[0], info_ref[1]
    for m, part in enumerate(parts):
        first = pl.multiple_of((col ^ m) * cols, cols)
        key = first + lax.broadcasted_iota(jnp.int32, (cols, queries), 0)
        key_bias = jnp.where(key < length, 0.0, -1e9).astype(f32)
        b = part[...].astype(f32)
        for h in range(heads):
            out_ref[pl.ds(first, cols), h * queries:(h + 1) * queries] = b[:, h, :].T + key_bias


def lay_bias(info, parts):
    queries, heads, cols = parts[0].shape
    shape = (len(parts) * cols, heads * queries)
    return pl.pallas_call(
        bias_kernel,
        grid_spec=pltpu.PrefetchScalarGridSpec(
            num_scalar_prefetch=1, grid=(1,),
            in_specs=[whole(p.shape) for p in parts], out_specs=whole(shape),
        ),
        out_shape=jax.ShapeDtypeStruct(shape, f32),
        compiler_params=VMEM_LIMIT,
        name="bias",
    )(info, *parts)


def attend_kernel(heads, sizes, info_ref, *refs):
    blocks = refs[:4]
    z_ref, bias_ref, wkv_ref, wqg_ref, wo_ref = refs[4:9]
    out_ref, k_s, vt_s, q_s, g_s, p_s, l_s, o_s = refs[-8:]
    step, cols, chan = z_ref.shape
    dim = chan // heads
    col, used = info_ref[0], info_ref[2]

    @pl.when(pl.program_id(0) == 0)
    def _():
        q_s[...] = jnp.zeros_like(q_s)

    def project(i, carry):
        rows = pl.ds(GROUP * i, GROUP)
        for p, ref in enumerate(blocks):
            first = pl.multiple_of((col ^ p) * cols, cols)
            kv = dot(ref[rows].reshape(GROUP * cols, chan), wkv_ref[...], NN).astype(bf16)
            k_s[rows, pl.ds(first, cols), :] = kv[:, :chan].reshape(GROUP, cols, chan)
            v = kv[:, chan:].reshape(GROUP, cols, chan)
            for r in range(GROUP):
                vt_s[GROUP * i + r, :, pl.ds(first, cols)] = v[r].T
        qg = dot(blocks[0][rows].reshape(GROUP * cols, chan), wqg_ref[...], NN)
        q = (qg[:, :chan] * dim ** -0.5).astype(bf16).reshape(GROUP, cols, chan)
        for r in range(GROUP):
            q_t = q[r].T
            for h in range(heads):
                q_s[GROUP * i + r, h * dim:(h + 1) * dim, h * cols:(h + 1) * cols] = q_t[h * dim:(h + 1) * dim]
        g_s[rows] = jax.nn.sigmoid(qg[:, chan:]).reshape(GROUP, cols, chan)
        return carry

    lax.fori_loop(0, step // GROUP, project, 0)

    def run(keys, shift):
        def weigh(r, slot):
            s = dot(k_s[r, :keys, :], q_s[r], NN) + bias_ref[:keys, :]
            e = jnp.exp(s - jnp.max(s, axis=0, keepdims=True) if shift else s)
            l_s[r] = jnp.sum(e, axis=0, keepdims=True)
            p_s[slot, :keys, :] = e.astype(bf16)

        def mix(r, slot):
            o = dot(vt_s[r, :, :keys], p_s[slot, :keys, :], NN)
            inv = 1.0 / l_s[r]
            for h in range(heads):
                part = o[h * dim:(h + 1) * dim, h * cols:(h + 1) * cols]
                o_s[r, h * dim:(h + 1) * dim, :] = part * inv[:, h * cols:(h + 1) * cols]

        def pair(i, carry):
            r = 2 * i
            weigh(r, 0)
            mix(lax.rem(r + step - 1, step), 1)
            weigh(r + 1, 1)
            mix(r, 0)
            return carry

        def single(r, carry):
            weigh(r, 0)
            mix(r, 0)
            return carry

        if shift:
            lax.fori_loop(0, step, single, 0)
        else:
            lax.fori_loop(0, step // 2, pair, 0)
            mix(step - 1, 1)

    for keys in sizes[:-1]:
        pl.when(used == keys)(functools.partial(run, keys, False))
    l = l_s[...]
    fine = (used < sizes[-1]) & (jnp.min(l) > SUM_RANGE[0]) & (jnp.max(l) < SUM_RANGE[1])
    pl.when(jnp.logical_not(fine))(functools.partial(run, sizes[-1], True))

    def finish(i, carry):
        rows = pl.ds(GROUP * i, GROUP)
        gated = jnp.concatenate([(o_s[GROUP * i + r].T * g_s[GROUP * i + r]).astype(bf16) for r in range(GROUP)], axis=0)
        update = dot(gated, wo_ref[...], NN).reshape(GROUP, cols, chan)
        out_ref[rows] = (z_ref[rows].astype(f32) + update).astype(bf16)
        return carry

    lax.fori_loop(0, step // GROUP, finish, 0)


def attend(heads, sizes, info, blocks, skips, z, bias, weights, prev, start, rows):
    cols, chan = z.shape[1:]
    step = ATTEND_ROWS
    first = start // step
    keys = 4 * cols
    here = [pl.BlockSpec((step, cols, chan), lambda i, _, skip=skip: (skip // step + i, 0, 0)) for skip in skips]
    there = pl.BlockSpec((step, cols, chan), lambda i, _: (first + i, 0, 0))
    args = [info] + list(blocks) + [z, bias] + list(weights)
    specs = here + [there, whole(bias.shape)] + [whole(w.shape) for w in weights]
    alias = {}
    if prev is not None:
        alias = {len(args): 0}
        args.append(prev)
        specs.append(pl.BlockSpec(memory_space=pl.ANY))
    return pl.pallas_call(
        functools.partial(attend_kernel, heads, sizes),
        grid_spec=pltpu.PrefetchScalarGridSpec(
            num_scalar_prefetch=1, grid=(rows // step,), in_specs=specs, out_specs=there,
            scratch_shapes=[
                pltpu.VMEM((step, keys, chan), bf16),
                pltpu.VMEM((step, chan, keys), bf16),
                pltpu.VMEM((step, chan, heads * cols), bf16),
                pltpu.VMEM((step, cols, chan), f32),
                pltpu.VMEM((2, keys, heads * cols), bf16),
                pltpu.VMEM((step, 1, heads * cols), f32),
                pltpu.VMEM((step, chan, cols), f32),
            ],
        ),
        out_shape=jax.ShapeDtypeStruct(z.shape, z.dtype),
        input_output_aliases=alias,
        compiler_params=pltpu.CompilerParams(vmem_limit_bytes=ATTEND_VMEM[prev is not None]),
        cost_estimate=pl.CostEstimate(flops=rows * cols * chan * 8000, bytes_accessed=rows * cols * chan * 12, transcendentals=0),
        name="attend",
    )(*args)


def solution(mesh):
    tile_spec = P(('dp', 'row'), 'col', None)
    num_cols = mesh.shape['col']
    x_pairs = [(c, c ^ 2) for c in range(num_cols)]
    core_pairs = [(c, c ^ 1) for c in range(num_cols)]

    def inner(z, res_mask, ln_gamma, ln_beta, w_q, w_k, w_v, w_b, w_g, w_o):
        _, cols, chan = z.shape
        heads = w_b.shape[1]
        sizes = (3 * cols, 7 * cols // 2, 4 * cols)
        col_idx = lax.axis_index('col')
        gamma, beta, wb_t = ln_gamma.reshape(1, chan), ln_beta.reshape(1, chan), w_b.T
        starts = [sum(CHUNKS[:i]) for i in range(len(CHUNKS))]
        first, bias_tile = normalize(z, gamma, beta, wb_t, None, 0, CHUNKS[:1], False)
        second, bias_tile = normalize(z, gamma, beta, wb_t, bias_tile, starts[1], CHUNKS[1:2], False)
        *others, bias_tile, rest = normalize(z, gamma, beta, wb_t, bias_tile, starts[2], CHUNKS[2:], True)
        own = [first, second] + others
        other_tile = lax.ppermute(bias_tile, 'row', [(0, 1), (1, 0)])
        info, w_kv, w_qg = make_plan(heads, sizes, res_mask.reshape(4, cols), gamma, beta, w_q, w_k, w_v, wb_t, w_g)
        weights = (w_kv, w_qg, w_o)

        halves = [bias_tile[:cols], bias_tile[cols:], other_tile[:cols], other_tile[cols:]]
        parts = []
        for m in range(num_cols):
            place = (col_idx ^ m) ^ (2 * lax.axis_index('row'))
            send = jnp.where(place & 2, jnp.where(place & 1, halves[3], halves[2]), jnp.where(place & 1, halves[1], halves[0]))
            parts.append(lax.ppermute(send, 'col', [(c, c ^ m) for c in range(num_cols)]) if m else send)
        bias = lay_bias(info, parts)
        far, near = [], []
        for a in own:
            far.append(lax.ppermute(a, 'col', x_pairs))
        for a in (first, second, rest):
            near.append(lax.ppermute(a, 'col', core_pairs))
        out = None
        for i, (start, rows) in enumerate(zip(starts, CHUNKS)):
            diag = lax.ppermute(far[i], 'col', core_pairs)
            out = attend(heads, sizes, info, (own[i], near[min(i, 2)], far[i], diag), (0, max(start - starts[2], 0) if i > 1 else 0, 0, 0), z, bias, weights, out, start, rows)
        return out

    return jax.shard_map(inner, mesh=mesh, in_specs=(tile_spec, P('dp'), P(), P(), P(), P(), P(), P(), P(), P()), out_specs=tile_spec, check_vma=False)
```

```python
import functools

import jax
import jax.numpy as jnp
from jax import lax
from jax.experimental import pallas as pl
from jax.experimental.pallas import tpu as pltpu
from jax.sharding import PartitionSpec as P


LN_EPS = 1e-5
CHUNKS = (16, 32, 48, 48, 48, 32, 32)
NORM_ROWS = 16
ATTEND_ROWS = 16
GROUP = 16
ATTEND_VMEM = 40 * 1024 * 1024
SCORE_BOUND = 1e8
VALUE_BOUND = 1e20
SUM_RANGE = (1e-10, 1e15)
NN = (((1,), (0,)), ((), ()))
NT = (((1,), (1,)), ((), ()))
f32, bf16 = jnp.float32, jnp.bfloat16
dot = functools.partial(lax.dot_general, preferred_element_type=f32)
VMEM_LIMIT = pltpu.CompilerParams(vmem_limit_bytes=67043328)


def whole(shape):
    return pl.BlockSpec(shape, lambda *_: (0,) * len(shape))


def plan_kernel(heads, sizes, mask_ref, gamma_ref, beta_ref, wq_ref, wk_ref, wv_ref, wb_ref, wg_ref, info_ref, wkv_ref, wqg_ref):
    chan = gamma_ref.shape[1]
    dim = chan // heads
    col_idx = lax.axis_index('col')
    wkv_ref[:, :chan], wkv_ref[:, chan:] = wk_ref[...], wv_ref[...]
    wqg_ref[:, :chan], wqg_ref[:, chan:] = wq_ref[...], wg_ref[...]
    reach = jnp.broadcast_to(jnp.abs(gamma_ref[...]) * chan ** 0.5 + jnp.abs(beta_ref[...]), (8, chan)) * 1.05
    q = jnp.dot(reach, jnp.abs(wq_ref[...].astype(f32)), preferred_element_type=f32) * dim ** -0.5
    k = jnp.dot(reach, jnp.abs(wk_ref[...].astype(f32)), preferred_element_type=f32)
    v = jnp.dot(reach, jnp.abs(wv_ref[...].astype(f32)), preferred_element_type=f32)
    b = reach[:1] * jnp.sum(jnp.abs(wb_ref[...].astype(f32)), axis=0, keepdims=True)
    s_bound = (jnp.sum(q * k) + jnp.sum(b)) * 1.1
    v_bound = jnp.max(v) * 1.1
    length = jnp.sum(mask_ref[...].astype(f32)).astype(jnp.int32)
    used = jnp.where(length <= sizes[0], sizes[0], sizes[1])
    info_ref[0] = col_idx
    info_ref[1] = length
    info_ref[2] = jnp.where((s_bound < SCORE_BOUND) & (v_bound < VALUE_BOUND), used, sizes[2])


def make_plan(heads, sizes, *args):
    chan = args[1].shape[1]
    return pl.pallas_call(
        functools.partial(plan_kernel, heads, sizes),
        in_specs=[whole(x.shape) for x in args],
        out_specs=[pl.BlockSpec(memory_space=pltpu.SMEM), whole((chan, 2 * chan)), whole((chan, 2 * chan))],
        out_shape=[jax.ShapeDtypeStruct((3,), jnp.int32)] + [jax.ShapeDtypeStruct((chan, 2 * chan), bf16)] * 2,
        compiler_params=VMEM_LIMIT,
        name="plan",
    )(*args)


def norm_kernel(places, aliased, z_ref, gamma_ref, beta_ref, wb_ref, *out_refs):
    out_refs = out_refs[1:] if aliased else out_refs
    rows, cols, chan = z_ref.shape
    b_ref = out_refs[len(places)]
    z = z_ref[...].reshape(rows * cols, chan)
    ones = jnp.full((chan, chan), 1.0 / chan, bf16)
    centered = z.astype(f32) - dot(z, ones, NN)
    var = jnp.mean(centered * centered, axis=-1, keepdims=True)
    a = (centered * lax.rsqrt(var + LN_EPS) * gamma_ref[...] + beta_ref[...]).astype(bf16)
    blocks = a.reshape(rows, cols, chan)
    i = pl.program_id(0)
    for out_ref, (lo, steps, offset) in zip(out_refs, places):
        @pl.when((i >= lo) & (i < lo + steps))
        def _():
            out_ref[...] = blocks[offset:offset + out_ref.shape[0]]
    for out_ref in out_refs[len(places) + 1:]:
        out_ref[...] = blocks
    b = dot(wb_ref[...], a, NT)
    for r in range(rows):
        b_ref[r] = b[:, r * cols:(r + 1) * cols].astype(bf16)


def normalize(z, gamma, beta, wb_t, prev, start, chunks, joined):
    total, cols, chan = z.shape
    heads = wb_t.shape[0]
    step = NORM_ROWS
    first = start // step
    rows = sum(chunks)
    places, specs = [], []
    for i, c in enumerate(chunks):
        lo, offset = divmod(sum(chunks[:i]), step)
        steps = max(c // step, 1)
        places.append((lo, steps, offset))
        specs.append(pl.BlockSpec((min(step, c), cols, chan), lambda i, lo=lo, steps=steps: (jnp.clip(i - lo, 0, steps - 1), 0, 0)))
    specs.append(pl.BlockSpec((step, heads, cols), lambda i: (first + i, 0, 0)))
    shapes = [jax.ShapeDtypeStruct((c, cols, chan), bf16) for c in chunks] + [jax.ShapeDtypeStruct((total, heads, cols), bf16)]
    if joined:
        specs.append(pl.BlockSpec((step, cols, chan), lambda i: (i, 0, 0)))
        shapes.append(jax.ShapeDtypeStruct((rows, cols, chan), bf16))
    args = [z, gamma, beta, wb_t]
    in_specs = [pl.BlockSpec((step, cols, chan), lambda i: (first + i, 0, 0))] + [whole(x.shape) for x in args[1:]]
    alias = {}
    if prev is not None:
        alias = {len(args): len(chunks)}
        args.append(prev)
        in_specs.append(pl.BlockSpec(memory_space=pl.ANY))
    return pl.pallas_call(
        functools.partial(norm_kernel, places, prev is not None),
        grid=(rows // step,),
        in_specs=in_specs,
        out_specs=specs,
        out_shape=shapes,
        input_output_aliases=alias,
        compiler_params=VMEM_LIMIT,
        cost_estimate=pl.CostEstimate(flops=rows * cols * chan * 300, bytes_accessed=rows * cols * chan * 4, transcendentals=0),
        name="norm",
    )(*args)


def bias_kernel(info_ref, *refs):
    parts, out_ref = refs[:-1], refs[-1]
    queries, heads, cols = parts[0].shape
    col, length = info_ref[0], info_ref[1]
    for m, part in enumerate(parts):
        first = pl.multiple_of((col ^ m) * cols, cols)
        key = first + lax.broadcasted_iota(jnp.int32, (cols, queries), 0)
        key_bias = jnp.where(key < length, 0.0, -1e9).astype(f32)
        b = part[...].astype(f32)
        for h in range(heads):
            out_ref[pl.ds(first, cols), h * queries:(h + 1) * queries] = b[:, h, :].T + key_bias


def lay_bias(info, parts):
    queries, heads, cols = parts[0].shape
    shape = (len(parts) * cols, heads * queries)
    return pl.pallas_call(
        bias_kernel,
        grid_spec=pltpu.PrefetchScalarGridSpec(
            num_scalar_prefetch=1, grid=(1,),
            in_specs=[whole(p.shape) for p in parts], out_specs=whole(shape),
        ),
        out_shape=jax.ShapeDtypeStruct(shape, f32),
        compiler_params=pltpu.CompilerParams(vmem_limit_bytes=ATTEND_VMEM),
        name="bias",
    )(info, *parts)


def attend_kernel(heads, sizes, info_ref, *refs):
    blocks = refs[:4]
    z_ref, bias_ref, wkv_ref, wqg_ref, wo_ref = refs[4:9]
    out_ref, k_s, vt_s, q_s, g_s, p_s, l_s, o_s = refs[-8:]
    step, cols, chan = z_ref.shape
    dim = chan // heads
    col, used = info_ref[0], info_ref[2]

    @pl.when(pl.program_id(0) == 0)
    def _():
        q_s[...] = jnp.zeros_like(q_s)

    def project(i, carry):
        rows = pl.ds(GROUP * i, GROUP)
        for p, ref in enumerate(blocks):
            first = pl.multiple_of((col ^ p) * cols, cols)
            kv = dot(ref[rows].reshape(GROUP * cols, chan), wkv_ref[...], NN).astype(bf16)
            k_s[rows, pl.ds(first, cols), :] = kv[:, :chan].reshape(GROUP, cols, chan)
            v = kv[:, chan:].reshape(GROUP, cols, chan)
            for r in range(GROUP):
                vt_s[GROUP * i + r, :, pl.ds(first, cols)] = v[r].T
        qg = dot(blocks[0][rows].reshape(GROUP * cols, chan), wqg_ref[...], NN)
        q = (qg[:, :chan] * dim ** -0.5).astype(bf16).reshape(GROUP, cols, chan)
        for r in range(GROUP):
            q_t = q[r].T
            for h in range(heads):
                q_s[GROUP * i + r, h * dim:(h + 1) * dim, h * cols:(h + 1) * cols] = q_t[h * dim:(h + 1) * dim]
        g_s[rows] = jax.nn.sigmoid(qg[:, chan:]).reshape(GROUP, cols, chan)
        return carry

    lax.fori_loop(0, step // GROUP, project, 0)

    def run(keys, shift):
        def weigh(r, slot):
            s = dot(k_s[r, :keys, :], q_s[r], NN) + bias_ref[:keys, :]
            e = jnp.exp(s - jnp.max(s, axis=0, keepdims=True) if shift else s)
            l_s[r] = jnp.sum(e, axis=0, keepdims=True)
            p_s[slot, :keys, :] = e.astype(bf16)

        def mix(r, slot):
            o = dot(vt_s[r, :, :keys], p_s[slot, :keys, :], NN)
            inv = 1.0 / l_s[r]
            for h in range(heads):
                part = o[h * dim:(h + 1) * dim, h * cols:(h + 1) * cols]
                o_s[r, h * dim:(h + 1) * dim, :] = part * inv[:, h * cols:(h + 1) * cols]

        def pair(i, carry):
            r = 2 * i
            weigh(r, 0)
            mix(lax.rem(r + step - 1, step), 1)
            weigh(r + 1, 1)
            mix(r, 0)
            return carry

        def single(r, carry):
            weigh(r, 0)
            mix(r, 0)
            return carry

        if shift:
            lax.fori_loop(0, step, single, 0)
        else:
            lax.fori_loop(0, step // 2, pair, 0)
            mix(step - 1, 1)

    for keys in sizes[:-1]:
        pl.when(used == keys)(functools.partial(run, keys, False))
    l = l_s[...]
    fine = (used < sizes[-1]) & (jnp.min(l) > SUM_RANGE[0]) & (jnp.max(l) < SUM_RANGE[1])
    pl.when(jnp.logical_not(fine))(functools.partial(run, sizes[-1], True))

    def finish(i, carry):
        rows = pl.ds(GROUP * i, GROUP)
        gated = jnp.concatenate([(o_s[GROUP * i + r].T * g_s[GROUP * i + r]).astype(bf16) for r in range(GROUP)], axis=0)
        update = dot(gated, wo_ref[...], NN).reshape(GROUP, cols, chan)
        out_ref[rows] = (z_ref[rows].astype(f32) + update).astype(bf16)
        return carry

    lax.fori_loop(0, step // GROUP, finish, 0)


def attend(heads, sizes, info, blocks, skips, z, bias, weights, prev, start, rows):
    cols, chan = z.shape[1:]
    step = ATTEND_ROWS
    first = start // step
    keys = 4 * cols
    here = [pl.BlockSpec((step, cols, chan), lambda i, _, skip=skip: (skip // step + i, 0, 0)) for skip in skips]
    there = pl.BlockSpec((step, cols, chan), lambda i, _: (first + i, 0, 0))
    args = [info] + list(blocks) + [z, bias] + list(weights)
    specs = here + [there, whole(bias.shape)] + [whole(w.shape) for w in weights]
    alias = {}
    if prev is not None:
        alias = {len(args): 0}
        args.append(prev)
        specs.append(pl.BlockSpec(memory_space=pl.ANY))
    return pl.pallas_call(
        functools.partial(attend_kernel, heads, sizes),
        grid_spec=pltpu.PrefetchScalarGridSpec(
            num_scalar_prefetch=1, grid=(rows // step,), in_specs=specs, out_specs=there,
            scratch_shapes=[
                pltpu.VMEM((step, keys, chan), bf16),
                pltpu.VMEM((step, chan, keys), bf16),
                pltpu.VMEM((step, chan, heads * cols), bf16),
                pltpu.VMEM((step, cols, chan), f32),
                pltpu.VMEM((2, keys, heads * cols), bf16),
                pltpu.VMEM((step, 1, heads * cols), f32),
                pltpu.VMEM((step, chan, cols), f32),
            ],
        ),
        out_shape=jax.ShapeDtypeStruct(z.shape, z.dtype),
        input_output_aliases=alias,
        compiler_params=pltpu.CompilerParams(vmem_limit_bytes=ATTEND_VMEM),
        cost_estimate=pl.CostEstimate(flops=rows * cols * chan * 8000, bytes_accessed=rows * cols * chan * 12, transcendentals=0),
        name="attend",
    )(*args)


def solution(mesh):
    tile_spec = P(('dp', 'row'), 'col', None)
    num_cols = mesh.shape['col']
    x_pairs = [(c, c ^ 2) for c in range(num_cols)]
    core_pairs = [(c, c ^ 1) for c in range(num_cols)]

    def inner(z, res_mask, ln_gamma, ln_beta, w_q, w_k, w_v, w_b, w_g, w_o):
        _, cols, chan = z.shape
        heads = w_b.shape[1]
        sizes = (3 * cols, 7 * cols // 2, 4 * cols)
        col_idx = lax.axis_index('col')
        gamma, beta, wb_t = ln_gamma.reshape(1, chan), ln_beta.reshape(1, chan), w_b.T
        starts = [sum(CHUNKS[:i]) for i in range(len(CHUNKS))]
        first, bias_tile = normalize(z, gamma, beta, wb_t, None, 0, CHUNKS[:1], False)
        second, bias_tile = normalize(z, gamma, beta, wb_t, bias_tile, starts[1], CHUNKS[1:2], False)
        *others, bias_tile, rest = normalize(z, gamma, beta, wb_t, bias_tile, starts[2], CHUNKS[2:], True)
        own = [first, second] + others
        other_tile = lax.ppermute(bias_tile, 'row', [(0, 1), (1, 0)])
        info, w_kv, w_qg = make_plan(heads, sizes, res_mask.reshape(4, cols), gamma, beta, w_q, w_k, w_v, wb_t, w_g)
        weights = (w_kv, w_qg, w_o)

        halves = [bias_tile[:cols], bias_tile[cols:], other_tile[:cols], other_tile[cols:]]
        parts = []
        for m in range(num_cols):
            place = (col_idx ^ m) ^ (2 * lax.axis_index('row'))
            send = jnp.where(place & 2, jnp.where(place & 1, halves[3], halves[2]), jnp.where(place & 1, halves[1], halves[0]))
            parts.append(lax.ppermute(send, 'col', [(c, c ^ m) for c in range(num_cols)]) if m else send)
        bias = lay_bias(info, parts)
        far, near = [], []
        for a in own:
            far.append(lax.ppermute(a, 'col', x_pairs))
        for a in (first, second, rest):
            near.append(lax.ppermute(a, 'col', core_pairs))
        out = None
        for i, (start, rows) in enumerate(zip(starts, CHUNKS)):
            diag = lax.ppermute(far[i], 'col', core_pairs)
            out = attend(heads, sizes, info, (own[i], near[min(i, 2)], far[i], diag), (0, max(start - starts[2], 0) if i > 1 else 0, 0, 0), z, bias, weights, out, start, rows)
        return out

    return jax.shard_map(inner, mesh=mesh, in_specs=(tile_spec, P('dp'), P(), P(), P(), P(), P(), P(), P(), P()), out_specs=tile_spec, check_vma=False)
```

```python
import functools

import jax
import jax.numpy as jnp
from jax import lax
from jax.experimental import pallas as pl
from jax.experimental.pallas import tpu as pltpu
from jax.sharding import PartitionSpec as P


LN_EPS = 1e-5
CHUNKS = (16, 32, 48, 48, 36, 28, 24, 24)
NORM_ROWS = 16
ATTEND_ROWS = 16
GROUP = 16
ATTEND_VMEM = 40 * 1024 * 1024
SCORE_BOUND = 1e8
VALUE_BOUND = 1e20
SUM_RANGE = (1e-10, 1e15)
NN = (((1,), (0,)), ((), ()))
NT = (((1,), (1,)), ((), ()))
f32, bf16 = jnp.float32, jnp.bfloat16
dot = functools.partial(lax.dot_general, preferred_element_type=f32)
VMEM_LIMIT = pltpu.CompilerParams(vmem_limit_bytes=67043328)


def whole(shape):
    return pl.BlockSpec(shape, lambda *_: (0,) * len(shape))


def plan_kernel(heads, sizes, mask_ref, gamma_ref, beta_ref, wq_ref, wk_ref, wv_ref, wb_ref, wg_ref, info_ref, wkv_ref, wqg_ref):
    chan = gamma_ref.shape[1]
    dim = chan // heads
    col_idx = lax.axis_index('col')
    wkv_ref[:, :chan], wkv_ref[:, chan:] = wk_ref[...], wv_ref[...]
    wqg_ref[:, :chan], wqg_ref[:, chan:] = wq_ref[...], wg_ref[...]
    reach = jnp.broadcast_to(jnp.abs(gamma_ref[...]) * chan ** 0.5 + jnp.abs(beta_ref[...]), (8, chan)) * 1.05
    q = jnp.dot(reach, jnp.abs(wq_ref[...].astype(f32)), preferred_element_type=f32) * dim ** -0.5
    k = jnp.dot(reach, jnp.abs(wk_ref[...].astype(f32)), preferred_element_type=f32)
    v = jnp.dot(reach, jnp.abs(wv_ref[...].astype(f32)), preferred_element_type=f32)
    b = reach[:1] * jnp.sum(jnp.abs(wb_ref[...].astype(f32)), axis=0, keepdims=True)
    s_bound = (jnp.sum(q * k) + jnp.sum(b)) * 1.1
    v_bound = jnp.max(v) * 1.1
    length = jnp.sum(mask_ref[...].astype(f32)).astype(jnp.int32)
    used = jnp.where(length <= sizes[0], sizes[0], sizes[1])
    info_ref[0] = col_idx
    info_ref[1] = length
    info_ref[2] = jnp.where((s_bound < SCORE_BOUND) & (v_bound < VALUE_BOUND), used, sizes[2])


def make_plan(heads, sizes, *args):
    chan = args[1].shape[1]
    return pl.pallas_call(
        functools.partial(plan_kernel, heads, sizes),
        in_specs=[whole(x.shape) for x in args],
        out_specs=[pl.BlockSpec(memory_space=pltpu.SMEM), whole((chan, 2 * chan)), whole((chan, 2 * chan))],
        out_shape=[jax.ShapeDtypeStruct((3,), jnp.int32)] + [jax.ShapeDtypeStruct((chan, 2 * chan), bf16)] * 2,
        compiler_params=VMEM_LIMIT,
        name="plan",
    )(*args)


def norm_kernel(places, aliased, z_ref, gamma_ref, beta_ref, wb_ref, *out_refs):
    out_refs = out_refs[1:] if aliased else out_refs
    rows, cols, chan = z_ref.shape
    b_ref = out_refs[len(places)]
    z = z_ref[...].reshape(rows * cols, chan)
    ones = jnp.full((chan, chan), 1.0 / chan, bf16)
    centered = z.astype(f32) - dot(z, ones, NN)
    var = jnp.mean(centered * centered, axis=-1, keepdims=True)
    a = (centered * lax.rsqrt(var + LN_EPS) * gamma_ref[...] + beta_ref[...]).astype(bf16)
    blocks = a.reshape(rows, cols, chan)
    i = pl.program_id(0)
    for out_ref, (lo, size) in zip(out_refs, places):
        if out_ref.shape[0] == rows:
            @pl.when((i * rows >= lo) & (i * rows < lo + size))
            def _():
                out_ref[...] = blocks
        else:
            for st in range(lo // rows, (lo + size - 1) // rows + 1):
                begin, end = max(lo, st * rows), min(lo + size, (st + 1) * rows)

                @pl.when(i == st)
                def _():
                    out_ref[begin - lo:end - lo] = blocks[begin - st * rows:end - st * rows]
    for out_ref in out_refs[len(places) + 1:]:
        out_ref[...] = blocks
    b = dot(wb_ref[...], a, NT)
    for r in range(rows):
        b_ref[r] = b[:, r * cols:(r + 1) * cols].astype(bf16)


def normalize(z, gamma, beta, wb_t, prev, start, chunks, joined):
    total, cols, chan = z.shape
    heads = wb_t.shape[0]
    step = NORM_ROWS
    first = start // step
    rows = sum(chunks)
    places, specs = [], []
    for i, c in enumerate(chunks):
        lo = sum(chunks[:i])
        places.append((lo, c))
        if lo % step or c % step:
            specs.append(whole((c, cols, chan)))
        else:
            specs.append(pl.BlockSpec((step, cols, chan), lambda i, lo=lo // step, n=c // step: (jnp.clip(i - lo, 0, n - 1), 0, 0)))
    specs.append(pl.BlockSpec((step, heads, cols), lambda i: (first + i, 0, 0)))
    shapes = [jax.ShapeDtypeStruct((c, cols, chan), bf16) for c in chunks] + [jax.ShapeDtypeStruct((total, heads, cols), bf16)]
    if joined:
        specs.append(pl.BlockSpec((step, cols, chan), lambda i: (i, 0, 0)))
        shapes.append(jax.ShapeDtypeStruct((rows, cols, chan), bf16))
    args = [z, gamma, beta, wb_t]
    in_specs = [pl.BlockSpec((step, cols, chan), lambda i: (first + i, 0, 0))] + [whole(x.shape) for x in args[1:]]
    alias = {}
    if prev is not None:
        alias = {len(args): len(chunks)}
        args.append(prev)
        in_specs.append(pl.BlockSpec(memory_space=pl.ANY))
    return pl.pallas_call(
        functools.partial(norm_kernel, places, prev is not None),
        grid=(rows // step,),
        in_specs=in_specs,
        out_specs=specs,
        out_shape=shapes,
        input_output_aliases=alias,
        compiler_params=VMEM_LIMIT,
        cost_estimate=pl.CostEstimate(flops=rows * cols * chan * 300, bytes_accessed=rows * cols * chan * 4, transcendentals=0),
        name="norm",
    )(*args)


def bias_kernel(info_ref, *refs):
    parts, out_ref = refs[:-1], refs[-1]
    queries, heads, cols = parts[0].shape
    col, length = info_ref[0], info_ref[1]
    for m, part in enumerate(parts):
        first = pl.multiple_of((col ^ m) * cols, cols)
        key = first + lax.broadcasted_iota(jnp.int32, (cols, queries), 0)
        key_bias = jnp.where(key < length, 0.0, -1e9).astype(f32)
        b = part[...].astype(f32)
        for h in range(heads):
            out_ref[pl.ds(first, cols), h * queries:(h + 1) * queries] = b[:, h, :].T + key_bias


def lay_bias(info, parts):
    queries, heads, cols = parts[0].shape
    shape = (len(parts) * cols, heads * queries)
    return pl.pallas_call(
        bias_kernel,
        grid_spec=pltpu.PrefetchScalarGridSpec(
            num_scalar_prefetch=1, grid=(1,),
            in_specs=[whole(p.shape) for p in parts], out_specs=whole(shape),
        ),
        out_shape=jax.ShapeDtypeStruct(shape, f32),
        compiler_params=pltpu.CompilerParams(vmem_limit_bytes=ATTEND_VMEM),
        name="bias",
    )(info, *parts)


def attend_kernel(heads, sizes, info_ref, *refs):
    blocks = refs[:4]
    z_ref, bias_ref, wkv_ref, wqg_ref, wo_ref = refs[4:9]
    out_ref, k_s, vt_s, q_s, g_s, p_s, l_s, o_s = refs[-8:]
    step, cols, chan = z_ref.shape
    group = GROUP if step % GROUP == 0 else step // 2
    dim = chan // heads
    col, used = info_ref[0], info_ref[2]

    @pl.when(pl.program_id(0) == 0)
    def _():
        q_s[...] = jnp.zeros_like(q_s)

    def project(i, carry):
        rows = pl.ds(group * i, group)
        for p, ref in enumerate(blocks):
            first = pl.multiple_of((col ^ p) * cols, cols)
            kv = dot(ref[rows].reshape(group * cols, chan), wkv_ref[...], NN).astype(bf16)
            k_s[rows, pl.ds(first, cols), :] = kv[:, :chan].reshape(group, cols, chan)
            v = kv[:, chan:].reshape(group, cols, chan)
            for r in range(group):
                vt_s[group * i + r, :, pl.ds(first, cols)] = v[r].T
        qg = dot(blocks[0][rows].reshape(group * cols, chan), wqg_ref[...], NN)
        q = (qg[:, :chan] * dim ** -0.5).astype(bf16).reshape(group, cols, chan)
        for r in range(group):
            q_t = q[r].T
            for h in range(heads):
                q_s[group * i + r, h * dim:(h + 1) * dim, h * cols:(h + 1) * cols] = q_t[h * dim:(h + 1) * dim]
        g_s[rows] = jax.nn.sigmoid(qg[:, chan:]).reshape(group, cols, chan)
        return carry

    lax.fori_loop(0, step // group, project, 0)

    def run(keys, shift):
        def weigh(r, slot):
            s = dot(k_s[r, :keys, :], q_s[r], NN) + bias_ref[:keys, :]
            e = jnp.exp(s - jnp.max(s, axis=0, keepdims=True) if shift else s)
            l_s[r] = jnp.sum(e, axis=0, keepdims=True)
            p_s[slot, :keys, :] = e.astype(bf16)

        def mix(r, slot):
            o = dot(vt_s[r, :, :keys], p_s[slot, :keys, :], NN)
            inv = 1.0 / l_s[r]
            for h in range(heads):
                part = o[h * dim:(h + 1) * dim, h * cols:(h + 1) * cols]
                o_s[r, h * dim:(h + 1) * dim, :] = part * inv[:, h * cols:(h + 1) * cols]

        def pair(i, carry):
            r = 2 * i
            weigh(r, 0)
            mix(lax.rem(r + step - 1, step), 1)
            weigh(r + 1, 1)
            mix(r, 0)
            return carry

        def single(r, carry):
            weigh(r, 0)
            mix(r, 0)
            return carry

        if shift:
            lax.fori_loop(0, step, single, 0)
        else:
            lax.fori_loop(0, step // 2, pair, 0)
            mix(step - 1, 1)

    for keys in sizes[:-1]:
        pl.when(used == keys)(functools.partial(run, keys, False))
    l = l_s[...]
    fine = (used < sizes[-1]) & (jnp.min(l) > SUM_RANGE[0]) & (jnp.max(l) < SUM_RANGE[1])
    pl.when(jnp.logical_not(fine))(functools.partial(run, sizes[-1], True))

    def finish(i, carry):
        rows = pl.ds(group * i, group)
        gated = jnp.concatenate([(o_s[group * i + r].T * g_s[group * i + r]).astype(bf16) for r in range(group)], axis=0)
        update = dot(gated, wo_ref[...], NN).reshape(group, cols, chan)
        out_ref[rows] = (z_ref[rows].astype(f32) + update).astype(bf16)
        return carry

    lax.fori_loop(0, step // group, finish, 0)


def attend(heads, sizes, info, blocks, skips, z, bias, weights, prev, start, rows):
    cols, chan = z.shape[1:]
    step = rows if rows % ATTEND_ROWS else ATTEND_ROWS
    keys = 4 * cols

    def at(skip):
        if skip % step == 0:
            return pl.BlockSpec((step, cols, chan), lambda i, _: (skip // step + i, 0, 0))
        return pl.BlockSpec((pl.Element(step), pl.Element(cols), pl.Element(chan)), lambda i, _: (skip + step * i, 0, 0))

    here, there = [at(skip) for skip in skips], at(start)
    args = [info] + list(blocks) + [z, bias] + list(weights)
    specs = here + [there, whole(bias.shape)] + [whole(w.shape) for w in weights]
    alias = {}
    if prev is not None:
        alias = {len(args): 0}
        args.append(prev)
        specs.append(pl.BlockSpec(memory_space=pl.ANY))
    return pl.pallas_call(
        functools.partial(attend_kernel, heads, sizes),
        grid_spec=pltpu.PrefetchScalarGridSpec(
            num_scalar_prefetch=1, grid=(rows // step,), in_specs=specs, out_specs=there,
            scratch_shapes=[
                pltpu.VMEM((step, keys, chan), bf16),
                pltpu.VMEM((step, chan, keys), bf16),
                pltpu.VMEM((step, chan, heads * cols), bf16),
                pltpu.VMEM((step, cols, chan), f32),
                pltpu.VMEM((2, keys, heads * cols), bf16),
                pltpu.VMEM((step, 1, heads * cols), f32),
                pltpu.VMEM((step, chan, cols), f32),
            ],
        ),
        out_shape=jax.ShapeDtypeStruct(z.shape, z.dtype),
        input_output_aliases=alias,
        compiler_params=pltpu.CompilerParams(vmem_limit_bytes=ATTEND_VMEM),
        cost_estimate=pl.CostEstimate(flops=rows * cols * chan * 8000, bytes_accessed=rows * cols * chan * 12, transcendentals=0),
        name="attend",
    )(*args)


def solution(mesh):
    tile_spec = P(('dp', 'row'), 'col', None)
    num_cols = mesh.shape['col']
    x_pairs = [(c, c ^ 2) for c in range(num_cols)]
    core_pairs = [(c, c ^ 1) for c in range(num_cols)]

    def inner(z, res_mask, ln_gamma, ln_beta, w_q, w_k, w_v, w_b, w_g, w_o):
        _, cols, chan = z.shape
        heads = w_b.shape[1]
        sizes = (3 * cols, 7 * cols // 2, 4 * cols)
        col_idx = lax.axis_index('col')
        gamma, beta, wb_t = ln_gamma.reshape(1, chan), ln_beta.reshape(1, chan), w_b.T
        starts = [sum(CHUNKS[:i]) for i in range(len(CHUNKS))]
        first, bias_tile = normalize(z, gamma, beta, wb_t, None, 0, CHUNKS[:1], False)
        second, bias_tile = normalize(z, gamma, beta, wb_t, bias_tile, starts[1], CHUNKS[1:2], False)
        *others, bias_tile, rest = normalize(z, gamma, beta, wb_t, bias_tile, starts[2], CHUNKS[2:], True)
        own = [first, second] + others
        other_tile = lax.ppermute(bias_tile, 'row', [(0, 1), (1, 0)])
        info, w_kv, w_qg = make_plan(heads, sizes, res_mask.reshape(4, cols), gamma, beta, w_q, w_k, w_v, wb_t, w_g)
        weights = (w_kv, w_qg, w_o)

        halves = [bias_tile[:cols], bias_tile[cols:], other_tile[:cols], other_tile[cols:]]
        parts = []
        for m in range(num_cols):
            place = (col_idx ^ m) ^ (2 * lax.axis_index('row'))
            send = jnp.where(place & 2, jnp.where(place & 1, halves[3], halves[2]), jnp.where(place & 1, halves[1], halves[0]))
            parts.append(lax.ppermute(send, 'col', [(c, c ^ m) for c in range(num_cols)]) if m else send)
        bias = lay_bias(info, parts)
        far, near = [], []
        for a in own:
            far.append(lax.ppermute(a, 'col', x_pairs))
        for a in (first, second, rest):
            near.append(lax.ppermute(a, 'col', core_pairs))
        out = None
        for i, (start, rows) in enumerate(zip(starts, CHUNKS)):
            diag = lax.ppermute(far[i], 'col', core_pairs)
            out = attend(heads, sizes, info, (own[i], near[min(i, 2)], far[i], diag), (0, max(start - starts[2], 0) if i > 1 else 0, 0, 0), z, bias, weights, out, start, rows)
        return out

    return jax.shard_map(inner, mesh=mesh, in_specs=(tile_spec, P('dp'), P(), P(), P(), P(), P(), P(), P(), P()), out_specs=tile_spec, check_vma=False)
```
